256 devices in a mesh: batch: 4 (over x), heads: 64 (over y, z, core).
Axes of the slice: x: 4, y: 4, z: 8, core: 2. Of those that a mesh axis runs over, the one named last changes fastest.
Arguments:
- draft_ids: int32 [192, 8], P('batch'), may hold values from 0 to 50279
- accepted: int32 [192], P('batch'), may hold values from 1 to 8
- embedding: bfloat16 [50280, 2560], P(None, 'heads'), may hold values from -6 to 6
- norm_gain: float32 [2, 2560], replicated, may hold values from 0.5 to 1.5
- w_zx: bfloat16 [2, 2560, 64, 128], P(None, None, 'heads'), may hold values from -0.125 to 0.125
- w_dt: bfloat16 [2, 2560, 64], P(None, None, 'heads'), may hold values from -0.125 to 0.125
- w_bc: bfloat16 [2, 2560, 256], P(None, None, 'heads'), may hold values from -0.125 to 0.125
- dt_bias: float32 [2, 64], P(None, 'heads'), may hold values from -4 to -1
- decay_rate: float32 [2, 64], P(None, 'heads'), may hold values from 1 to 16
- skip_weight: float32 [2, 64], P(None, 'heads'), may hold values from 0.5 to 1.5
- conv_x_w: bfloat16 [2, 4, 4096], P(None, None, 'heads'), may hold values from -3 to 3
- conv_x_b: bfloat16 [2, 4096], P(None, 'heads'), may hold values from -3 to 3
- conv_bc_w: bfloat16 [2, 4, 256], P(None, None, 'heads'), may hold values from -3 to 3
- conv_bc_b: bfloat16 [2, 256], P(None, 'heads'), may hold values from -3 to 3
- gate_gain: float32 [2, 4096], P(None, 'heads'), may hold values from 0.5 to 1.5
- out_w: bfloat16 [2, 4096, 2560], P(None, 'heads'), may hold values from -0.25 to 0.25
- ssm_state: float32 [2, 192, 64, 64, 128], P(None, 'batch', 'heads'), may hold values from -1.6 to 1.6
- conv_x_state: bfloat16 [2, 192, 3, 4096], P(None, 'batch', None, 'heads'), may hold values from -6 to 6
- conv_bc_state: bfloat16 [2, 192, 3, 256], P(None, 'batch', None, 'heads'), may hold values from -6 to 6
Outputs:
- hidden_out: bfloat16 [1536, 2560], P('batch', 'heads')
- new_ssm: float32 [2, 192, 64, 64, 128], P(None, 'batch', 'heads')
- new_conv_x: bfloat16 [2, 192, 3, 4096], P(None, 'batch', None, 'heads')
- new_conv_bc: bfloat16 [2, 192, 3, 256], P(None, 'batch', None, 'heads')
The draws below stay inside these ranges and needn't reach their ends.
Inputs may be any that keep to these rules, and one draw needn't show every extreme that they name: `accepted`: the number of a sequence's draft tokens that are kept, counted from the first.
All inputs are finite; a program needn't handle non-finite values.
Results may differ from the reference program's by a relative error of at most 0.015.
Values may be sent and summed in bfloat16 or wider, within the bound.
No kernel may reach another device: no remote copies, remote signals or barrier semaphores. Data moves between devices by JAX's collectives and lax.ppermute only.
A program may use at most 128 MiB of HBM per device.

```python
import math
import jax
import jax.numpy as jnp
import numpy as np
from jax import lax

D = 2560
P_SIZE = 64
N = 128
VOCAB = 50280
KCONV = 4
DRAFT = 8
LAYERS = 2
HEADS = 64
INNER = 4096
SEQS = 192


def set_ends(drawn, own_key, least, top_value):
    dims = drawn.shape
    index_at = [jax.random.randint(jax.random.fold_in(own_key, axis), (), 0, dims[axis]) for axis in range(len(dims))]
    drawn = drawn.at[tuple(index_at)].set(least)
    longest = dims.index(max(dims))
    index_at[longest] = (index_at[longest] + 1) % dims[longest]
    return drawn.at[tuple(index_at)].set(top_value)


def strengthened(values, key, source, target, shards_of, factor):
    owner, partner = [(jnp.arange(values.shape[position]) // (values.shape[position] // shards_of)).reshape([-1 if axis == position else 1 for axis in range(values.ndim)]) for position in (source, target)]
    chosen = jax.random.permutation(key, shards_of)[partner]
    strong = (owner == chosen) | (owner == (partner + shards_of // 2) % shards_of)
    return jnp.where(strong, factor * values, values)


def shard_levels(own_key, dims, split, low, largest):
    def one(axis_at, parts):
        heights = jax.random.uniform(jax.random.fold_in(jax.random.fold_in(own_key, 6), axis_at), (parts,), jnp.float32, low / len(split), largest / len(split))
        return jnp.repeat(jnp.exp(heights), dims[axis_at] // parts).reshape((-1,) + (1,) * (len(dims) - axis_at - 1))

    gain = one(*split[0])
    for cut in split[1:]:
        gain = gain * one(*cut)
    return gain


def rank_table(number_of, lean):
    loads = [(1 << 20) // math.isqrt(grade ** lean) + 1 for grade in range(1, number_of + 1)]
    scale = 1 + sum(loads) // (1 << 30)
    return np.cumsum(np.array([max(1, weight // scale) for weight in loads]))


def ranked_ids(stream_key, dims, amount, slope):
    listing = rank_table(amount, slope)
    ticket = jax.random.randint(jax.random.fold_in(stream_key, 1), dims, 0, int(listing[amount - 1]))
    grade = jnp.searchsorted(jnp.asarray(listing, jnp.int32), ticket, side="right")
    return jax.random.permutation(jax.random.fold_in(stream_key, 2), amount)[grade].astype(jnp.int32)


def centred(rng, dims, scale, bound, cuts=(), kind=jnp.bfloat16):
    result = scale * jax.random.normal(rng, dims, jnp.float32)
    if cuts:
        result = result * shard_levels(rng, dims, cuts, -0.22, 0.18)
    return jnp.clip(result, -bound, bound).astype(kind)


def bell_draw_with(key, shape, scale, bound, cuts, heavy, kind=jnp.bfloat16):
    array = scale * jax.random.normal(key, shape, jnp.float32)
    if cuts:
        array = array * shard_levels(key, shape, cuts, -0.22, 0.18)
    return jnp.clip(strengthened(array, jax.random.fold_in(key, 3), *heavy), -bound, bound).astype(kind)


def setup_inputs(seed: int = 0) -> dict:
    seeds = jax.random.split(jax.random.key(seed), 20)
    return {
        "draft_ids": set_ends(ranked_ids(seeds[0], (SEQS, DRAFT), VOCAB, 2), jax.random.fold_in(seeds[0], 3), 0, VOCAB - 1).astype(jnp.int32),
        "accepted": set_ends(jax.random.randint(seeds[1], (SEQS,), 1, DRAFT + 1), jax.random.fold_in(seeds[1], 1), 1, DRAFT).astype(jnp.int32),
        "embedding": centred(seeds[2], (VOCAB, D), 1.0, 6.0, ((1, 64),)),
        "norm_gain": jnp.clip(1.0 + 0.1 * jax.random.normal(seeds[3], (LAYERS, D), jnp.float32), 0.5, 1.5),
        "w_zx": centred(seeds[4], (LAYERS, D, HEADS, 2 * P_SIZE), D ** -0.5, 0.125, ((2, 64),)),
        "w_dt": centred(seeds[5], (LAYERS, D, HEADS), D ** -0.5, 0.125, ((2, 64),)),
        "w_bc": centred(seeds[6], (LAYERS, D, 2 * N), D ** -0.5, 0.125, ((2, 64),)),
        "dt_bias": jnp.clip(-4.0 + 3.0 * jax.random.uniform(seeds[7], (LAYERS, HEADS), jnp.float32) ** shard_levels(seeds[7], (LAYERS, HEADS), ((1, 64),), -0.2, 0.2), -4.0, -1.0),
        "decay_rate": jnp.clip(jnp.exp(math.log(16.0) - 2.7725887 * jax.random.uniform(seeds[8], (LAYERS, HEADS), jnp.float32) ** shard_levels(seeds[8], (LAYERS, HEADS), ((1, 64),), -0.2, 0.2)), 1.0, 16.0),
        "skip_weight": jnp.clip(0.5 + 1.0 * jax.random.uniform(seeds[9], (LAYERS, HEADS), jnp.float32) ** shard_levels(seeds[9], (LAYERS, HEADS), ((1, 64),), -0.2, 0.2), 0.5, 1.5),
        "conv_x_w": centred(seeds[10], (LAYERS, KCONV, INNER), 0.5, 3.0, ((2, 64),)),
        "conv_x_b": centred(seeds[11], (LAYERS, INNER), 0.5, 3.0, ((1, 64),)),
        "conv_bc_w": centred(seeds[12], (LAYERS, KCONV, 2 * N), 0.5, 3.0, ((2, 64),)),
        "conv_bc_b": centred(seeds[13], (LAYERS, 2 * N), 0.5, 3.0, ((1, 64),)),
        "gate_gain": jnp.clip(1.0 + 0.1 * jax.random.normal(seeds[14], (LAYERS, INNER), jnp.float32), 0.5, 1.5),
        "out_w": bell_draw_with(seeds[15], (LAYERS, INNER, D), INNER ** -0.5, 0.25, ((1, 64),), (1, 2, 64, 4.0)),
        "ssm_state": centred(seeds[16], (LAYERS, SEQS, HEADS, P_SIZE, N), 0.2, 1.6, ((1, 4), (2, 64)), jnp.float32),
        "conv_x_state": centred(seeds[17], (LAYERS, SEQS, KCONV - 1, INNER), 1.0, 6.0, ((1, 4), (3, 64))),
        "conv_bc_state": centred(seeds[18], (LAYERS, SEQS, KCONV - 1, 2 * N), 1.0, 6.0, ((1, 4), (3, 64))),
    }


EPS = 1e-05

def rms_scale(total, count):
    return lax.rsqrt(total / count + EPS)

def convolve(window, weight, bias, count):
    weight = weight.astype(jnp.float32)
    acc = window[:, 0:count] * weight[0]
    for k in range(1, weight.shape[0]):
        acc = acc + window[:, k:k + count] * weight[k]
    return jax.nn.silu(acc + bias.astype(jnp.float32))

def keep_rows(window, accepted, kept_rows):
    last_start = window.shape[1] - kept_rows
    kept = window[:, 1:1 + kept_rows]
    for start in range(2, last_start + 1):
        kept = jnp.where((accepted == start)[:, None, None], window[:, start:start + kept_rows], kept)
    return kept

def recur(decay, step, values, bmat, cmat, skip, state, accepted):
    kept = state
    outputs = []
    for t in range(values.shape[1]):
        state = decay[:, t, None, None] * state + (step[:, t, None] * values[:, t])[:, :, None] * bmat[:, t, None, :]
        outputs.append(lax.optimization_barrier(jnp.sum(state * cmat[:, t, None, :], axis=-1)) + skip * values[:, t])
        kept = jnp.where((accepted == t + 1)[:, None, None], state, kept)
    return (jnp.stack(outputs, 1), kept)

def reference(draft_ids, accepted, embedding, norm_gain, w_zx, w_dt, w_bc, dt_bias, decay_rate, skip_weight, conv_x_w, conv_x_b, conv_bc_w, conv_bc_b, gate_gain, out_w, ssm_state, conv_x_state, conv_bc_state):
    seqs, draft = draft_ids.shape
    heads = w_zx.shape[2]
    width = w_zx.shape[3] // 2
    inner = heads * width
    model = embedding.shape[1]
    states = w_bc.shape[2] // 2
    kernel = conv_x_w.shape[1]
    stream = embedding[draft_ids.reshape(-1)]
    saved_state, saved_x, saved_bc = ([], [], [])
    for layer in range(LAYERS):
        value = stream.astype(jnp.float32)
        normed = (value * rms_scale(lax.optimization_barrier(jnp.sum(value * value, -1, keepdims=True)), model) * norm_gain[layer]).astype(jnp.bfloat16)
        zx = jnp.dot(normed, w_zx[layer].reshape(model, -1), preferred_element_type=jnp.float32).astype(jnp.bfloat16)
        zx = zx.reshape(seqs, draft, heads, 2, width)
        gate_z = zx[:, :, :, 0].astype(jnp.float32)
        values = zx[:, :, :, 1].reshape(seqs, draft, inner)
        dt_raw = jnp.dot(normed, w_dt[layer], preferred_element_type=jnp.float32).astype(jnp.bfloat16).reshape(seqs, draft, heads)
        bc = jnp.dot(normed, w_bc[layer], preferred_element_type=jnp.float32).astype(jnp.bfloat16).reshape(seqs, draft, 2 * states)
        window_x = jnp.concatenate([conv_x_state[layer], values], axis=1)
        xc = convolve(window_x.astype(jnp.float32), conv_x_w[layer], conv_x_b[layer], draft).reshape(seqs, draft, heads, width)
        window_bc = jnp.concatenate([conv_bc_state[layer], bc], axis=1)
        bcc = convolve(window_bc.astype(jnp.float32), conv_bc_w[layer], conv_bc_b[layer], draft).astype(jnp.bfloat16)
        bcc = lax.optimization_barrier(bcc).astype(jnp.float32)
        bmat = bcc[..., :states]
        cmat = bcc[..., states:]
        step = jax.nn.softplus(dt_raw.astype(jnp.float32) + dt_bias[layer])
        decay = jnp.exp(-step * decay_rate[layer])

        def run(pieces):
            return recur(pieces[0], pieces[1], pieces[2], bmat, cmat, pieces[3], pieces[4], accepted)
        outputs, kept = lax.map(run, (jnp.moveaxis(decay, 2, 0), jnp.moveaxis(step, 2, 0), jnp.moveaxis(xc, 2, 0), skip_weight[layer], jnp.moveaxis(ssm_state[layer], 1, 0)))
        outputs = jnp.moveaxis(outputs, 0, 2)
        saved_state.append(jnp.moveaxis(kept, 0, 1))
        saved_x.append(keep_rows(window_x, accepted, kernel - 1))
        saved_bc.append(keep_rows(window_bc, accepted, kernel - 1))
        gated = outputs * jax.nn.silu(gate_z)
        ssq = lax.optimization_barrier(jnp.sum(gated * gated, axis=(2, 3))).reshape(-1)
        u = (gated.reshape(seqs, draft, inner) * gate_gain[layer]).astype(jnp.bfloat16).reshape(-1, inner)
        mix = jnp.dot(u, out_w[layer], preferred_element_type=jnp.float32) * rms_scale(ssq, inner)[:, None]
        stream = (stream.astype(jnp.float32) + mix).astype(jnp.bfloat16)
    return (stream, jnp.stack(saved_state), jnp.stack(saved_x), jnp.stack(saved_bc))
```

```python
import jax
import jax.numpy as jnp
from jax import lax
from jax.experimental import pallas as pl
from jax.experimental.pallas import tpu as pltpu
from jax.sharding import PartitionSpec as P

LAYERS = 2
EPS = 1e-05
BF = jnp.bfloat16
F32 = jnp.float32
LANES = 128

YS, ZS, CS = 4, 8, 2


def device_at(y, z, c):
    return (y * ZS + z) * CS + c


Z_GROUPS = [[device_at(y, z, c) for z in range(ZS)] for y in range(YS) for c in range(CS)]
Y_GROUPS = [[device_at(y, z, c) for y in range(YS)] for z in range(ZS) for c in range(CS)]
PARTNER = [(i, i ^ 1) for i in range(YS * ZS * CS)]


def swap_cores(value):
    return lax.ppermute(value, "heads", PARTNER)


def exchange(value, groups):
    return lax.all_to_all(value, "heads", 0, 0, tiled=True, axis_index_groups=groups)


def spread(value, groups):
    count = len(groups[0])
    return exchange(jnp.broadcast_to(value[None], (count, *value.shape)), groups)


def gather_planes(piece):
    rows, width = piece.shape
    over_z = spread(piece, Z_GROUPS)
    over_y = spread(over_z, Y_GROUPS)
    own = over_y.reshape(YS * ZS, rows, width)
    return own, swap_cores(own)


VMEM = pl.BlockSpec(memory_space=pltpu.VMEM)
SMEM = pl.BlockSpec(memory_space=pltpu.SMEM)
HBM = pl.BlockSpec(memory_space=pl.ANY)


def limit(mib):
    return pltpu.CompilerParams(vmem_limit_bytes=mib * 1024 * 1024)


def silu(v):
    return v / (1.0 + jnp.exp(-v))


def softplus(v):
    e = jnp.exp(-jnp.abs(v))
    grown = 1.0 + e
    small = grown == 1.0
    log1p = jnp.where(small, e, jnp.log(grown) * (e / jnp.where(small, 1.0, grown - 1.0)))
    return jnp.maximum(v, 0.0) + log1p


def lookup_kernel(ids_ref, table_ref, out_ref, tail_ref, acc_ref):
    rows, vocab = table_ref.shape
    tokens = acc_ref.shape[1]
    whole = vocab // LANES
    tail_at = whole * LANES
    lane = lax.broadcasted_iota(jnp.int32, (rows, LANES), 1)
    tail_ref[...] = jnp.zeros_like(tail_ref)
    if tail_at < vocab:
        tail_ref[:, : vocab - tail_at] = table_ref[:, tail_at:].astype(F32)
    tail = tail_ref[...]
    for tile in range(tokens // LANES):

        def one(i, acc, tile=tile):
            token = ids_ref[0, tile * LANES + i]
            block = jnp.minimum(token // LANES, whole - 1)
            at = pl.multiple_of(block * LANES, LANES)
            found = table_ref[:, pl.ds(at, LANES)].astype(F32)
            found = jnp.where(token >= tail_at, tail, found)
            moved = pltpu.roll(found, (i - token % LANES + LANES) % LANES, 1)
            return jnp.where(lane == i, moved, acc)

        acc = lax.fori_loop(0, LANES, one, jnp.zeros((rows, LANES), F32), unroll=8)
        acc_ref[:, tile * LANES : (tile + 1) * LANES] = acc
    for j in range(rows // 8):
        out_ref[:, j * tokens : (j + 1) * tokens] = acc_ref[8 * j : 8 * j + 8, :].astype(BF)


def lookup(ids, table):
    rows = table.shape[0]
    tokens = ids.shape[1]
    return pl.pallas_call(
        lookup_kernel,
        out_shape=jax.ShapeDtypeStruct((8, rows // 8 * tokens), BF),
        in_specs=[SMEM, VMEM],
        out_specs=VMEM,
        scratch_shapes=[pltpu.VMEM((rows, LANES), F32), pltpu.VMEM((rows, tokens), F32)],
        compiler_params=limit(12),
        name="lookup",
    )(ids, table)


def tdot(a, b):
    return lax.dot_general(a, b, (((0,), (0,)), ((), ())), preferred_element_type=F32)


def ndot(a, b):
    return lax.dot_general(a, b, (((1,), (1,)), ((), ())), preferred_element_type=F32)


def mdot(a, b):
    return lax.dot_general(a, b, (((1,), (0,)), ((), ())), preferred_element_type=F32)


def make_layer_kernel(layer, tokens, seqs, draft, own_cols, taps, has_base):
    model = own_cols * YS * ZS * CS
    pieces = own_cols // 8
    kept = taps - 1
    stream_lanes = pieces * tokens

    def kernel(*refs):
        (
            core_ref, scalar_ref, own_ref, oth_ref, wown_ref, woth_ref, gain_ref, zx_ref,
            small_ref, cols_ref, statex_ref, statebc_ref, acc_col_ref, acc_row_ref, outw_ref,
            ssm_ref,
        ) = refs[:16]
        rest = refs[17:] if has_base else refs[16:]
        (
            keep_ref, send_ref, newx_ref, newbc_ref, newssm_ref,
            xs, nb, h_in, h_out, xw_all, sem_in, sem_out,
        ) = rest
        core = core_ref[0]
        first = core == 0
        bias_dt = scalar_ref[0, layer]
        rate = scalar_ref[1, layer]
        skip = scalar_ref[2, layer]
        load = pltpu.make_async_copy(ssm_ref.at[layer], h_in, sem_in)
        load.start()

        total = jnp.zeros((8, tokens), F32)
        for k in range(YS * ZS):
            for j in range(pieces):
                lanes = slice(j * tokens, (j + 1) * tokens)
                a = own_ref[k, :, lanes].astype(F32)
                b = oth_ref[k, :, lanes].astype(F32)
                total = total + a * a + b * b
                at = 2 * k * own_cols + 8 * j
                xs[at : at + 8, :] = jnp.where(first, a, b)
                xs[at + own_cols : at + own_cols + 8, :] = jnp.where(first, b, a)
        scale = lax.rsqrt(jnp.sum(total, axis=0, keepdims=True) / model + EPS)
        gains = jnp.transpose(gain_ref[...])
        for j in range(model // LANES):
            at = slice(j * LANES, (j + 1) * LANES)
            col = gains[:, layer * (model // LANES) + j :][:, :1]
            nb[at, :] = ((xs[at, :] * scale) * col).astype(BF)

        normed = nb[...]
        take_own = core == layer
        wl = wown_ref.shape[2] - (model + 2 * LANES)
        states = YS * ZS * 8 // 2

        def bc_rows(lo, hi):
            a = wown_ref[:, :, lo + wl : hi + wl].astype(F32)
            b = woth_ref[:, :, lo + wl : hi + wl].astype(F32)
            return jnp.where(take_own, a, b).reshape(2 * states, hi - lo)

        zx = tdot(zx_ref[layer], normed).astype(BF)
        bc = mdot(bc_rows(0, model).astype(BF), normed).astype(BF).astype(F32)
        mine = mdot(small_ref[layer], normed).astype(BF)
        width = zx.shape[0] // 2
        gate_z = zx[:width].astype(F32)
        values = zx[width:].astype(F32)
        cols = cols_ref[layer]

        lane = lax.broadcasted_iota(jnp.int32, (1, tokens), 1)
        t0 = lane % draft

        def saved_at(j):
            seq = lax.broadcasted_iota(jnp.int32, (seqs, tokens), 0)
            at = lax.broadcasted_iota(jnp.int32, (seqs, tokens), 1)
            return (at == seq * draft + (draft - kept) + j).astype(F32).astype(BF)

        places = [saved_at(j) for j in range(kept)]
        place = jnp.concatenate(places, axis=0)
        before_x = sum(tdot(statex_ref[layer, j], places[j]) for j in range(kept))
        extra = bc_rows(model, model + 2 * LANES)
        before_bc = mdot(extra[:, : kept * seqs].astype(BF), place)
        before_mine = mdot(statebc_ref[layer], place)

        def convolve(now, before, weights, bias):
            acc = None
            for k in range(taps):
                d = taps - 1 - k
                if d:
                    shifted = jnp.where(
                        t0 >= d,
                        pltpu.roll(now, d, 1),
                        pltpu.roll(before, tokens - (draft - d), 1),
                    )
                else:
                    shifted = now
                term = shifted * weights[k]
                acc = term if acc is None else acc + term
            return silu(acc + bias)

        xc = convolve(values, before_x, [cols[:, k : k + 1] for k in range(taps)], cols[:, taps : taps + 1])
        base = kept * seqs
        bcc = convolve(
            bc,
            before_bc,
            [extra[:, base + k : base + k + 1] for k in range(taps)],
            extra[:, base + taps : base + taps + 1],
        ).astype(BF)

        acc_col = acc_col_ref[...]
        seq = lax.broadcasted_iota(jnp.int32, (seqs, tokens), 0)
        at = lax.broadcasted_iota(jnp.int32, (seqs, tokens), 1)
        values_b, before_b = zx[width:], before_x.astype(BF)
        before_mb = before_mine.astype(BF)
        for i in range(kept):
            row = acc_col + i
            new = ((at == seq * draft + row - kept) & (row >= kept)).astype(F32).astype(BF)
            old = ((at == seq * draft + (draft - kept) + row) & (row < kept)).astype(F32).astype(BF)
            newx_ref[i] = (ndot(new, values_b) + ndot(old, before_b)).astype(BF)
            newbc_ref[i] = (ndot(mine, new) + ndot(before_mb, old)).astype(BF)

        step = softplus(mine[4:5, :].astype(F32) + bias_dt)
        cum = step
        for d in (1, 2, 4):
            cum = cum + jnp.where(t0 >= d, pltpu.roll(cum, d, 1), 0.0)
        accepted = acc_row_ref[...]
        cut = jnp.where(t0 < accepted, step, 0.0)
        for d in (1, 2, 4):
            cut = cut + jnp.where((t0 & d) != 0, pltpu.roll(cut, d, 1), pltpu.roll(cut, tokens - d, 1))
        weight = jnp.where(t0 < accepted, jnp.exp(-rate * (cut - cum)) * step, 0.0)
        fall = jnp.exp(-rate * cum)
        fall_cut = jnp.exp(-rate * cut)
        xb = xc.astype(BF)
        xw_all[...] = (xc * weight).astype(BF)
        load.wait()

        per_tile = LANES // draft
        sub = lax.broadcasted_iota(jnp.int32, (LANES, LANES), 0)
        lan = lax.broadcasted_iota(jnp.int32, (LANES, LANES), 1)
        causal = (sub // draft == lan // draft) & (sub <= lan)
        group = lax.broadcasted_iota(jnp.int32, (1, LANES), 1) // draft
        pick16 = lax.broadcasted_iota(jnp.int32, (per_tile, LANES), 0) * draft == (
            lax.broadcasted_iota(jnp.int32, (per_tile, LANES), 1)
        )
        parts = []
        for tile in range(tokens // LANES):
            ls = slice(tile * LANES, (tile + 1) * LANES)
            bmat = bcc[:states, ls]
            cmat = bcc[states:, ls]
            cum_r = jnp.broadcast_to(cum[:, ls], (LANES, LANES))
            step_c = jnp.transpose(jnp.broadcast_to(step[:, ls], (LANES, LANES)))
            cum_c = jnp.transpose(cum_r)
            gram = tdot(bmat, cmat)
            within = jnp.where(causal, gram * (jnp.exp(-rate * (cum_r - cum_c)) * step_c), 0.0)
            y_new = mdot(xb[:, ls], within.astype(BF))
            y_old = jnp.zeros((width, LANES), F32)
            falls = jnp.sum(jnp.where(pick16, fall_cut[:, ls], 0.0), axis=1, keepdims=True)
            xw = xw_all[:, ls]
            for s in range(per_tile):
                n = tile * per_tile + s
                h0 = h_in[n]
                here = group == s
                y_old = jnp.where(here, mdot(h0.astype(BF), cmat), y_old)
                add = ndot(jnp.where(here, xw, jnp.zeros_like(xw)), bmat)
                h_out[n] = h0 * falls[s : s + 1, :] + add
            parts.append(fall[:, ls] * y_old + y_new)
        store = pltpu.make_async_copy(h_out, newssm_ref.at[layer], sem_out)
        store.start()
        y = jnp.concatenate(parts, axis=1) + skip * xc
        gated = y * silu(gate_z)
        ssq = jnp.sum(gated * gated, axis=0, keepdims=True)
        u = (gated * cols[:, taps + 1 : taps + 2]).astype(BF)

        high = ssq.astype(BF)
        low = (ssq - high.astype(F32)).astype(BF)
        row8 = lax.broadcasted_iota(jnp.int32, (8, tokens), 0)
        tail = jnp.where(row8 == 0, high.astype(F32), jnp.where(row8 == 1, low.astype(F32), 0.0))
        block = own_cols * CS * ZS
        for y_at in range(YS):
            out = tdot(outw_ref[layer, :, y_at * block : (y_at + 1) * block], u)
            out = out.reshape(ZS, CS, pieces, 8, tokens)
            for z in range(ZS):
                even, odd = out[z, 0], out[z, 1]
                rows = slice(z * pieces, (z + 1) * pieces)
                keep_ref[y_at, rows] = jnp.where(first, even, odd)
                send_ref[y_at, rows] = jnp.where(first, odd, even).astype(BF)
            keep_ref[y_at, ZS * pieces] = tail
            send_ref[y_at, ZS * pieces] = tail.astype(BF)
        store.wait()

    return kernel


def add_cores_kernel(keep_ref, got_ref, out_ref):
    tiles = keep_ref.shape[1]
    for y in range(YS):
        out_ref[y, : tiles - 1] = (
            keep_ref[y, : tiles - 1] + got_ref[y, : tiles - 1].astype(F32)
        ).astype(BF)
    tail = keep_ref[0, tiles - 1] + got_ref[0, tiles - 1].astype(F32)
    for y in range(YS):
        out_ref[y, tiles - 1] = split_tail(tail)


def split_tail(tail):
    row8 = lax.broadcasted_iota(jnp.int32, tail.shape, 0)
    ssq = tail[0:1] + tail[1:2]
    high = ssq.astype(BF).astype(F32)
    return jnp.where(row8 == 0, high, jnp.where(row8 == 1, ssq - high, 0.0)).astype(BF)


def add_y_kernel(got_ref, out_ref):
    tiles = got_ref.shape[1]
    pieces = (tiles - 1) // ZS

    def summed(rows):
        acc = got_ref[0, rows].astype(F32)
        for y in range(1, YS):
            acc = acc + got_ref[y, rows].astype(F32)
        return acc

    tail = split_tail(summed(slice(tiles - 1, tiles))[0])
    for z in range(ZS):
        out_ref[z, :pieces] = summed(slice(z * pieces, (z + 1) * pieces)).astype(BF)
        out_ref[z, pieces] = tail


def make_finish_kernel(inner, last):
    def finish_kernel(got_ref, stream_ref, out_ref):
        tiles = got_ref.shape[1]
        tokens = got_ref.shape[3]
        acc = got_ref[0].astype(F32)
        for z in range(1, ZS):
            acc = acc + got_ref[z].astype(F32)
        ssq = acc[tiles - 1, 0:1] + acc[tiles - 1, 1:2]
        scale = lax.rsqrt(ssq / inner + EPS)
        for j in range(tiles - 1):
            lanes = slice(j * tokens, (j + 1) * tokens)
            new = (stream_ref[:, lanes].astype(F32) + acc[j] * scale).astype(BF)
            if last:
                out_ref[j] = new
            else:
                out_ref[:, lanes] = new

    return finish_kernel


def call(kernel, out_shape, count, name):
    return pl.pallas_call(
        kernel,
        out_shape=out_shape,
        in_specs=[VMEM] * count,
        out_specs=VMEM,
        compiler_params=limit(10),
        name=name,
    )


def local(
    draft_ids,
    accepted,
    embedding,
    norm_gain,
    w_zx,
    w_dt,
    w_bc,
    dt_bias,
    decay_rate,
    skip_weight,
    conv_x_w,
    conv_x_b,
    conv_bc_w,
    conv_bc_b,
    gate_gain,
    out_w,
    ssm_state,
    conv_x_state,
    conv_bc_state,
):
    seqs, draft = draft_ids.shape
    tokens = seqs * draft
    own_cols = embedding.shape[1]
    model = own_cols * YS * ZS * CS
    width = w_zx.shape[3] // 2
    inner = width * YS * ZS * CS
    bc_here = w_bc.shape[2]
    taps = conv_x_w.shape[1]
    kept = taps - 1
    pieces = own_cols // 8
    states = ssm_state.shape[4]
    core = lax.axis_index("heads") % CS

    w_rows = jnp.swapaxes(w_bc, 1, 2)
    state_rows = jnp.transpose(conv_bc_state, (0, 3, 2, 1)).reshape(LAYERS, bc_here, kept * seqs)
    tap_rows = jnp.swapaxes(conv_bc_w, 1, 2)
    room = 2 * LANES - kept * seqs - taps - 1
    bc_rows = jnp.concatenate(
        [w_rows, state_rows, tap_rows, conv_bc_b[:, :, None], jnp.zeros((LAYERS, bc_here, room), BF)],
        axis=2,
    )
    first = core == 0
    kept_rows = jnp.where(first, bc_rows[0], bc_rows[1])
    got_rows = swap_cores(jnp.where(first, bc_rows[1], bc_rows[0]))
    pair_rows = jnp.concatenate(
        [jnp.where(first, kept_rows, got_rows), jnp.where(first, got_rows, kept_rows)], axis=0
    )

    small = jnp.concatenate(
        [w_rows, jnp.swapaxes(w_dt, 1, 2), jnp.zeros((LAYERS, 7 - bc_here, model), BF)], axis=1
    )
    state_own = jnp.pad(state_rows, ((0, 0), (0, 8 - bc_here), (0, 0)))
    cols = jnp.stack(
        [conv_x_w[:, k].astype(F32) for k in range(taps)]
        + [conv_x_b.astype(F32), gate_gain]
        + [jnp.zeros_like(gate_gain)] * (6 - taps),
        axis=2,
    )
    gains = jnp.pad(norm_gain.reshape(-1, LANES), ((0, LANES - LAYERS * model // LANES), (0, 0)))
    scalars = jnp.stack([dt_bias[:, 0], decay_rate[:, 0], skip_weight[:, 0]])
    acc_col = accepted[:, None]
    acc_row = jnp.repeat(accepted, draft)[None]
    state_x = jnp.swapaxes(conv_x_state, 1, 2)
    states_in = ssm_state.reshape(LAYERS, seqs, width, states)
    zx_w = w_zx.reshape(LAYERS, model, 2 * width)

    stream = lookup(draft_ids.reshape(1, tokens), embedding.T)
    own, oth = gather_planes(jnp.concatenate([stream, pair_rows], axis=1))
    w_own, w_oth = own, oth
    new_ssm = None
    new_x, new_bc = [], []
    tiles = ZS * pieces + 1
    for layer in range(LAYERS):
        args = [
            core.reshape(1), scalars, own, oth, w_own, w_oth, gains, zx_w,
            small, cols, state_x, state_own, acc_col, acc_row, out_w, states_in,
        ]
        specs = [SMEM, SMEM] + [VMEM] * 13 + [HBM]
        aliases = {}
        if new_ssm is not None:
            args.append(new_ssm)
            specs.append(HBM)
            aliases = {16: 4}
        keep, send, x_rows, bc_kept, new_ssm = pl.pallas_call(
            make_layer_kernel(layer, tokens, seqs, draft, own_cols, taps, new_ssm is not None),
            out_shape=(
                jax.ShapeDtypeStruct((YS, tiles, 8, tokens), F32),
                jax.ShapeDtypeStruct((YS, tiles, 8, tokens), BF),
                jax.ShapeDtypeStruct((kept, seqs, width), BF),
                jax.ShapeDtypeStruct((kept, 8, seqs), BF),
                jax.ShapeDtypeStruct(states_in.shape, F32),
            ),
            in_specs=specs,
            out_specs=(VMEM, VMEM, VMEM, VMEM, HBM),
            scratch_shapes=[
                pltpu.VMEM((model, tokens), F32),
                pltpu.VMEM((model, tokens), BF),
                pltpu.VMEM(states_in.shape[1:], F32),
                pltpu.VMEM(states_in.shape[1:], F32),
                pltpu.VMEM((width, tokens), BF),
                pltpu.SemaphoreType.DMA,
                pltpu.SemaphoreType.DMA,
            ],
            input_output_aliases=aliases,
            compiler_params=limit(34),
            name=f"layer_{layer}",
        )(*args)
        new_x.append(x_rows)
        new_bc.append(bc_kept[:, :bc_here])
        summed = call(
            add_cores_kernel, jax.ShapeDtypeStruct((YS, tiles, 8, tokens), BF), 2, "add_cores"
        )(keep, swap_cores(send))
        summed = call(
            add_y_kernel, jax.ShapeDtypeStruct((ZS, pieces + 1, 8, tokens), BF), 1, "add_y"
        )(exchange(summed, Y_GROUPS))
        last = layer + 1 == LAYERS
        shape = (pieces, 8, tokens) if last else (8, pieces * tokens)
        stream = call(
            make_finish_kernel(inner, last), jax.ShapeDtypeStruct(shape, BF), 2, "finish"
        )(exchange(summed, Z_GROUPS), stream)
        if not last:
            own, oth = gather_planes(stream)
    hidden = stream.reshape(own_cols, tokens).T
    kept_x = jnp.swapaxes(jnp.stack(new_x), 1, 2)
    kept_bc = jnp.transpose(jnp.stack(new_bc), (0, 3, 1, 2))
    return (hidden, new_ssm.reshape(ssm_state.shape), kept_x, kept_bc)


def solution(mesh):
    placed = (
        P("batch", None),
        P("batch"),
        P(None, "heads"),
        P(),
        P(None, None, "heads", None),
        P(None, None, "heads"),
        P(None, None, "heads"),
        P(None, "heads"),
        P(None, "heads"),
        P(None, "heads"),
        P(None, None, "heads"),
        P(None, "heads"),
        P(None, None, "heads"),
        P(None, "heads"),
        P(None, "heads"),
        P(None, "heads", None),
        P(None, "batch", "heads", None, None),
        P(None, "batch", None, "heads"),
        P(None, "batch", None, "heads"),
    )
    return jax.shard_map(
        local,
        mesh=mesh,
        in_specs=placed,
        out_specs=(
            P("batch", "heads"),
            P(None, "batch", "heads", None, None),
            P(None, "batch", None, "heads"),
            P(None, "batch", None, "heads"),
        ),
        check_vma=False,
    )
```

```python
import jax
import jax.numpy as jnp
from jax import lax
from jax.experimental import pallas as pl
from jax.experimental.pallas import tpu as pltpu
from jax.sharding import PartitionSpec as P


LAYERS = 2
EPS = 1e-05
BF = jnp.bfloat16
F32 = jnp.float32
LANES = 128

YS, ZS, CS = 4, 8, 2
XS = 4


def device_at(y, z, c):
    return (y * ZS + z) * CS + c


Z_GROUPS = [[device_at(y, z, c) for z in range(ZS)] for y in range(YS) for c in range(CS)]
Y_GROUPS = [[device_at(y, z, c) for y in range(YS)] for z in range(ZS) for c in range(CS)]
PARTNER = [(i, i ^ 1) for i in range(YS * ZS * CS)]


PLACES = [(x, y, z, c) for x in range(XS) for y in range(YS) for z in range(ZS) for c in range(CS)]


def index_of(x, y, z, c):
    return x * YS * ZS * CS + device_at(y % YS, z % ZS, c)


def fetch(value, source):
    pairs = [(index_of(*source(*place)), index_of(*place)) for place in PLACES]
    return lax.ppermute(value, ("batch", "heads"), pairs)


def swap_cores(value):
    return lax.ppermute(value, "heads", PARTNER)


def exchange(value, groups):
    return lax.all_to_all(value, "heads", 0, 0, tiled=True, axis_index_groups=groups)


def spread(value, groups):
    count = len(groups[0])
    return exchange(jnp.broadcast_to(value[None], (count, *value.shape)), groups)


def gather_planes(piece):
    rows, width = piece.shape
    over_z = spread(piece, Z_GROUPS)
    over_y = spread(over_z, Y_GROUPS)
    own = over_y.reshape(YS * ZS, rows, width)
    return own, swap_cores(own)


VMEM = pl.BlockSpec(memory_space=pltpu.VMEM)
SMEM = pl.BlockSpec(memory_space=pltpu.SMEM)
HBM = pl.BlockSpec(memory_space=pltpu.HBM)


def limit(mib):
    return pltpu.CompilerParams(vmem_limit_bytes=mib * 1024 * 1024)


def silu(v):
    return v / (1.0 + jnp.exp(-v))


def softplus(v):
    e = jnp.exp(-jnp.abs(v))
    grown = 1.0 + e
    small = grown == 1.0
    log1p = jnp.where(small, e, jnp.log(grown) * (e / jnp.where(small, 1.0, grown - 1.0)))
    return jnp.maximum(v, 0.0) + log1p


SHIFT = LANES.bit_length() - 1


def position():
    at = lax.axis_index("heads")
    return lax.axis_index("batch"), at // (ZS * CS), at // CS % ZS, at % CS


def lookup_kernel(ids_ref, table_ref, beside_ref, out_ref, tail_ref, acc_ref):
    rows, vocab = table_ref.shape
    draft = ids_ref.shape[0]
    tokens = acc_ref.shape[1]
    whole = vocab // LANES
    tail_at = whole * LANES
    lane = lax.broadcasted_iota(jnp.int32, (rows, LANES), 1)
    tail_ref[...] = jnp.zeros_like(tail_ref)
    if tail_at < vocab:
        tail_ref[:, : vocab - tail_at] = table_ref[:, tail_at:].astype(F32)
    tail = tail_ref[...]
    seqs_a_tile = LANES // draft
    for tile in range(tokens // LANES):

        def one(s, acc, tile=tile):
            for t in range(draft):
                token = ids_ref[t, tile * seqs_a_tile + s]
                i = s * draft + t
                block = jnp.minimum(token >> SHIFT, whole - 1)
                at = pl.multiple_of(block << SHIFT, LANES)
                found = table_ref[:, pl.ds(at, LANES)].astype(F32)
                found = jnp.where(token >= tail_at, tail, found)
                moved = pltpu.roll(found, (i - token) & (LANES - 1), 1)
                acc = jnp.where(lane == i, moved, acc)
            return acc

        acc = lax.fori_loop(0, seqs_a_tile, one, jnp.zeros((rows, LANES), F32), unroll=2)
        acc_ref[:, tile * LANES : (tile + 1) * LANES] = acc
    for j in range(rows // 8):
        out_ref[:, j * tokens : (j + 1) * tokens] = acc_ref[8 * j : 8 * j + 8, :].astype(BF)
    out_ref[:, rows // 8 * tokens :] = beside_ref[...]


def lookup(ids, table, beside):
    rows = table.shape[0]
    tokens = ids.size
    return pl.pallas_call(
        lookup_kernel,
        out_shape=jax.ShapeDtypeStruct((8, rows // 8 * tokens + beside.shape[1]), BF),
        in_specs=[SMEM, VMEM, VMEM],
        out_specs=VMEM,
        scratch_shapes=[pltpu.VMEM((rows, LANES), F32), pltpu.VMEM((rows, tokens), F32)],
        compiler_params=limit(12),
        name="lookup",
    )(ids, table, beside)


def tdot(a, b):
    return lax.dot_general(a, b, (((0,), (0,)), ((), ())), preferred_element_type=F32)


def ndot(a, b):
    return lax.dot_general(a, b, (((1,), (1,)), ((), ())), preferred_element_type=F32)


def mdot(a, b):
    return lax.dot_general(a, b, (((1,), (0,)), ((), ())), preferred_element_type=F32)


SLOT = 64
AT_TAPS, AT_ACCEPTED, AT_BIAS, AT_RATE, AT_SKIP = 24, 32, 33, 34, 35


def saved_at(j, kept, seqs, draft):
    seq = lax.broadcasted_iota(jnp.int32, (seqs, seqs * draft), 0)
    at = lax.broadcasted_iota(jnp.int32, (seqs, seqs * draft), 1)
    return (at == seq * draft + (draft - kept) + j).astype(F32).astype(BF)


def setup_kernel(
    bias_ref, rate_ref, skip_ref, w_ref, wdt_ref, state_ref, taps_ref, tapb_ref, gain_ref,
    xtaps_ref, xtapb_ref, gate_ref, statex_ref, accepted_ref,
    keep_ref, send_ref, table_ref, own8_ref, beforex_ref, beforebc_ref, spread_ref, table,
):
    model = w_ref.shape[2]
    here = w_ref.shape[1]
    kept, seqs = state_ref.shape[1], state_ref.shape[3]
    draft = spread_ref.shape[1] // seqs
    taps = taps_ref.shape[1]
    width = xtaps_ref.shape[2]
    first = position()[3] == 0
    places = [saved_at(j, kept, seqs, draft) for j in range(kept)]
    outs, rows = [], []
    for layer in range(LAYERS):
        table[...] = jnp.zeros_like(table)
        table[0:taps, 0:here] = taps_ref[layer].astype(F32)
        table[taps : taps + 1, 0:here] = tapb_ref[layer : layer + 1].astype(F32)
        turned = jnp.transpose(table[...])[:8]
        tiles = []
        for j in range(kept):
            table[...] = jnp.zeros_like(table)
            table[0:here, 0:seqs] = state_ref[layer, j].astype(F32)
            tiles.append(table[0:8, :])
        outs.append((turned, tiles[0] + pltpu.roll(tiles[1], SLOT, 1), tiles[2]))
        row = w_ref[layer].astype(F32)
        rows.append(jnp.concatenate([row, jnp.zeros((8 - here, model), F32)], axis=0))
        own8_ref[layer] = jnp.concatenate(
            [row, wdt_ref[layer : layer + 1, :].astype(F32), jnp.zeros((7 - here, model), F32)], axis=0
        ).astype(BF)
    for ref, pick in ((keep_ref, first), (send_ref, jnp.logical_not(first))):
        for lo, values in (
            (0, rows),
            (model, [o[0] for o in outs]),
            (model + LANES, [o[1] for o in outs]),
            (model + 2 * LANES, [o[2] for o in outs]),
        ):
            value = jnp.where(pick, values[0], values[1])
            value = jnp.where(first, value, pltpu.roll(value, here, 0))
            ref[:, lo : lo + value.shape[1]] = value.astype(BF)
    for layer in range(LAYERS):
        table[...] = jnp.zeros_like(table)
        for j in range(model // LANES):
            table[j : j + 1, :] = gain_ref[layer : layer + 1, j * LANES : (j + 1) * LANES]
        table[AT_TAPS : AT_TAPS + taps, :width] = xtaps_ref[layer].astype(F32)
        table[AT_TAPS + taps : AT_TAPS + taps + 1, :width] = xtapb_ref[layer : layer + 1].astype(F32)
        table[AT_TAPS + taps + 1 : AT_TAPS + taps + 2, :width] = gate_ref[layer : layer + 1]
        table[AT_ACCEPTED : AT_ACCEPTED + 1, :seqs] = accepted_ref[...].astype(F32)
        table[AT_BIAS : AT_BIAS + 1, :] = jnp.full((1, LANES), bias_ref[0, layer], F32)
        table[AT_RATE : AT_RATE + 1, :] = jnp.full((1, LANES), rate_ref[0, layer], F32)
        table[AT_SKIP : AT_SKIP + 1, :] = jnp.full((1, LANES), skip_ref[0, layer], F32)
        table_ref[layer] = jnp.transpose(table[...])
        beforex_ref[layer] = sum(tdot(statex_ref[layer, j], places[j]) for j in range(kept)).astype(BF)
        beforebc_ref[layer] = jnp.concatenate(
            [
                sum(mdot(state_ref[layer, j], places[j]) for j in range(kept)),
                jnp.zeros((8 - here, seqs * draft), F32),
            ],
            axis=0,
        ).astype(BF)
    seq = lax.broadcasted_iota(jnp.int32, (seqs, seqs * draft), 0)
    at = lax.broadcasted_iota(jnp.int32, (seqs, seqs * draft), 1)
    owner = (at // draft == seq).astype(F32).astype(BF)
    spread_ref[...] = mdot(
        jnp.broadcast_to(accepted_ref[...].astype(F32), (8, seqs)).astype(BF), owner
    ).astype(jnp.int32)


def pair_kernel(keep_ref, got_ref, rows_ref, states_ref):
    cut = rows_ref.shape[1]
    rows_ref[...] = (keep_ref[:, :cut].astype(F32) + got_ref[:, :cut].astype(F32)).astype(BF)
    states_ref[...] = (keep_ref[:, cut:].astype(F32) + got_ref[:, cut:].astype(F32)).astype(BF)


def join_kernel(*refs):
    *pieces, out_ref = refs
    at = 0
    for piece in pieces:
        count = piece.shape[0]
        out_ref[at : at + count] = piece[...]
        at += count


def join(pieces):
    shape = (sum(p.shape[0] for p in pieces), *pieces[0].shape[1:])
    return call(join_kernel, jax.ShapeDtypeStruct(shape, BF), len(pieces))(*pieces)


def make_layer_kernel(layer, tokens, seqs, draft, own_cols, taps, last):
    model = own_cols * YS * ZS * CS
    pieces = own_cols // 8
    kept = taps - 1

    def kernel(*refs):
        own_ref, oth_ref, sown_ref, soth_ref, *w_refs = refs[: 4 + 2 * XS]
        (
            table_ref, own8_ref, beforex_ref, beforebc_ref, spread_ref, zx_ref, outw_ref, ssm_ref,
        ) = refs[4 + 2 * XS : 12 + 2 * XS]
        rest = refs[12 + 2 * XS :]
        if last:
            old_x_ref, old_bc_ref, _, *rest = rest
        (
            keep_ref, send_ref, newx_ref, newbc_ref, newssm_ref,
            xs, nb, wb, h_in, h_out, xw_all, zx_w, out_w, sems,
        ) = rest
        x_at, y_at0, z_at0, core = position()
        first = core == 0
        load_w = pltpu.make_async_copy(zx_ref.at[layer], zx_w, sems.at[0])
        load = pltpu.make_async_copy(ssm_ref.at[layer], h_in, sems.at[1])
        load_o = pltpu.make_async_copy(outw_ref.at[layer], out_w, sems.at[2])
        load_w.start()
        load.start()
        load_o.start()

        turned = table_ref[layer]
        width = beforex_ref.shape[1]
        here = newbc_ref.shape[-2]
        acc_col = turned[:seqs, AT_ACCEPTED : AT_ACCEPTED + 1].astype(jnp.int32)
        cols = turned[:width, AT_TAPS : AT_TAPS + 8]
        bias_dt = turned[:1, AT_BIAS : AT_BIAS + 1]
        rate = turned[:1, AT_RATE : AT_RATE + 1]
        skip = turned[:1, AT_SKIP : AT_SKIP + 1]

        take_own = core == layer
        for dx in range(XS):
            at_x = lax.rem(x_at + dx, XS)
            for dy in range(YS):
                at_y = lax.rem(y_at0 + dy, YS)
                for j in range(2):
                    at_z = lax.rem(z_at0 + 2 * at_x + j, ZS)
                    block = jnp.where(take_own, w_refs[dx][dy * 2 + j], w_refs[XS + dx][dy * 2 + j])
                    wb[at_y * ZS + at_z] = block

        total = jnp.zeros((8, tokens), F32)
        for k in range(YS * ZS):
            for j in range(pieces):
                lanes = slice(j * tokens, (j + 1) * tokens)
                a = own_ref[k, :, lanes].astype(F32)
                b = oth_ref[k, :, lanes].astype(F32)
                total = total + a * a + b * b
                at = 2 * k * own_cols + 8 * j
                xs[at : at + 8, :] = jnp.where(first, a, b)
                xs[at + own_cols : at + own_cols + 8, :] = jnp.where(first, b, a)
        scale = lax.rsqrt(jnp.sum(total, axis=0, keepdims=True) / model + EPS)
        for j in range(model // LANES):
            at = slice(j * LANES, (j + 1) * LANES)
            col = turned[:, j : j + 1]
            nb[at, :] = ((xs[at, :] * scale) * col).astype(BF)

        normed = nb[...]
        states = YS * ZS * 8 // 2

        def bc_rows(lo, hi):
            return wb[:, :, lo:hi].astype(F32).reshape(2 * states, hi - lo)

        mine = mdot(own8_ref[layer], normed).astype(BF)
        bc = mdot(bc_rows(0, model).astype(BF), normed).astype(BF).astype(F32)
        load_w.wait()
        zx = tdot(zx_w[...], normed).astype(BF)
        gate_z = zx[:width].astype(F32)
        values = zx[width:].astype(F32)

        lane = lax.broadcasted_iota(jnp.int32, (1, tokens), 1)
        t0 = lane % draft

        slot = lax.broadcasted_iota(jnp.int32, (2 * LANES, tokens), 0)
        slot_lane = lax.broadcasted_iota(jnp.int32, (2 * LANES, tokens), 1)
        slot_seq, slot_j = slot & (SLOT - 1), slot // SLOT
        place = (
            (slot_seq < seqs) & (slot_j < kept) & (slot_lane == slot_seq * draft + (draft - kept) + slot_j)
        ).astype(F32).astype(BF)
        lanes = slice(pieces * tokens, pieces * tokens + 2 * LANES)
        saved_bc = jnp.where(
            take_own, sown_ref[:, :, lanes].astype(F32), soth_ref[:, :, lanes].astype(F32)
        ).reshape(2 * states, 2 * LANES)
        before_bc = mdot(saved_bc.astype(BF), place)
        extra = bc_rows(model, model + LANES)
        before_b, before_mb = beforex_ref[layer], beforebc_ref[layer]
        before_x = before_b.astype(F32)

        def convolve(now, before, weights, bias):
            acc = None
            for k in range(taps):
                d = taps - 1 - k
                if d:
                    shifted = jnp.where(
                        t0 >= d,
                        pltpu.roll(now, d, 1),
                        pltpu.roll(before, tokens - (draft - d), 1),
                    )
                else:
                    shifted = now
                term = shifted * weights[k]
                acc = term if acc is None else acc + term
            return silu(acc + bias)

        xc = convolve(values, before_x, [cols[:, k : k + 1] for k in range(taps)], cols[:, taps : taps + 1])
        bcc = convolve(
            bc,
            before_bc,
            [extra[:, k : k + 1] for k in range(taps)],
            extra[:, taps : taps + 1],
        ).astype(BF)

        seq = lax.broadcasted_iota(jnp.int32, (seqs, tokens), 0)
        at = lax.broadcasted_iota(jnp.int32, (seqs, tokens), 1)
        values_b = zx[width:]
        for i in range(kept):
            row = acc_col + i
            new = ((at == seq * draft + row - kept) & (row >= kept)).astype(F32).astype(BF)
            old = ((at == seq * draft + (draft - kept) + row) & (row < kept)).astype(F32).astype(BF)
            rows_x = (ndot(new, values_b) + ndot(old, before_b)).astype(BF)
            rows_bc = (ndot(mine, new) + ndot(before_mb, old))[:here].astype(BF)
            if last:
                newx_ref[layer, i], newbc_ref[layer, i] = rows_x, rows_bc
                for l in range(layer):
                    newx_ref[l, i], newbc_ref[l, i] = old_x_ref[i], old_bc_ref[i]
            else:
                newx_ref[i], newbc_ref[i] = rows_x, rows_bc

        step = softplus(mine[here : here + 1, :].astype(F32) + bias_dt)
        cum = step
        for d in (1, 2, 4):
            cum = cum + jnp.where(t0 >= d, pltpu.roll(cum, d, 1), 0.0)
        accepted = spread_ref[:1]
        cut = jnp.where(t0 < accepted, step, 0.0)
        for d in (1, 2, 4):
            cut = cut + jnp.where((t0 & d) != 0, pltpu.roll(cut, d, 1), pltpu.roll(cut, tokens - d, 1))
        weight = jnp.where(t0 < accepted, jnp.exp(-rate * (cut - cum)) * step, 0.0)
        fall = jnp.exp(-rate * cum)
        fall_cut = jnp.exp(-rate * cut)
        xb = xc.astype(BF)
        xw_all[...] = (xc * weight).astype(BF)
        load.wait()

        per_tile = LANES // draft
        sub = lax.broadcasted_iota(jnp.int32, (LANES, LANES), 0)
        lan = lax.broadcasted_iota(jnp.int32, (LANES, LANES), 1)
        causal = (sub // draft == lan // draft) & (sub <= lan)
        group = lax.broadcasted_iota(jnp.int32, (1, LANES), 1) // draft
        pick16 = lax.broadcasted_iota(jnp.int32, (per_tile, LANES), 0) * draft == (
            lax.broadcasted_iota(jnp.int32, (per_tile, LANES), 1)
        )
        parts = []
        for tile in range(tokens // LANES):
            ls = slice(tile * LANES, (tile + 1) * LANES)
            bmat = bcc[:states, ls]
            cmat = bcc[states:, ls]
            cum_r = jnp.broadcast_to(cum[:, ls], (LANES, LANES))
            step_c = jnp.transpose(jnp.broadcast_to(step[:, ls], (LANES, LANES)))
            cum_c = jnp.transpose(cum_r)
            gram = tdot(bmat, cmat)
            within = jnp.where(causal, gram * (jnp.exp(-rate * (cum_r - cum_c)) * step_c), 0.0)
            y_new = mdot(xb[:, ls], within.astype(BF))
            y_old = jnp.zeros((width, LANES), F32)
            falls = jnp.sum(jnp.where(pick16, fall_cut[:, ls], 0.0), axis=1, keepdims=True)
            xw = xw_all[:, ls]
            for s in range(per_tile):
                n = tile * per_tile + s
                h0 = h_in[n]
                here = group == s
                y_old = jnp.where(here, mdot(h0.astype(BF), cmat), y_old)
                add = ndot(jnp.where(here, xw, jnp.zeros_like(xw)), bmat)
                h_out[n] = h0 * falls[s : s + 1, :] + add
            parts.append(fall[:, ls] * y_old + y_new)
        store = pltpu.make_async_copy(h_out, newssm_ref.at[layer], sems.at[3])
        store.start()
        y = jnp.concatenate(parts, axis=1) + skip * xc
        gated = y * silu(gate_z)
        ssq = jnp.sum(gated * gated, axis=0, keepdims=True)
        u = (gated * cols[:, taps + 1 : taps + 2]).astype(BF)

        high = ssq.astype(BF)
        low = (ssq - high.astype(F32)).astype(BF)
        row8 = lax.broadcasted_iota(jnp.int32, (8, tokens), 0)
        tail = jnp.where(row8 == 0, high.astype(F32), jnp.where(row8 == 1, low.astype(F32), 0.0))
        block = own_cols * CS * ZS
        load_o.wait()
        for y_at in range(YS):
            out = tdot(out_w[:, y_at * block : (y_at + 1) * block], u)
            out = out.reshape(ZS, CS, pieces, 8, tokens)
            for z in range(ZS):
                even, odd = out[z, 0], out[z, 1]
                rows = slice(z * pieces, (z + 1) * pieces)
                keep_ref[y_at, rows] = jnp.where(first, even, odd)
                send_ref[y_at, rows] = jnp.where(first, odd, even).astype(BF)
            keep_ref[y_at, ZS * pieces] = tail
            send_ref[y_at, ZS * pieces] = tail.astype(BF)
        store.wait()

    return kernel


def add_cores_kernel(keep_ref, got_ref, out_ref):
    tiles = keep_ref.shape[1]
    for y in range(YS):
        out_ref[y, : tiles - 1] = (
            keep_ref[y, : tiles - 1] + got_ref[y, : tiles - 1].astype(F32)
        ).astype(BF)
    tail = keep_ref[0, tiles - 1] + got_ref[0, tiles - 1].astype(F32)
    for y in range(YS):
        out_ref[y, tiles - 1] = split_tail(tail)


def split_tail(tail):
    row8 = lax.broadcasted_iota(jnp.int32, tail.shape, 0)
    ssq = tail[0:1] + tail[1:2]
    high = ssq.astype(BF).astype(F32)
    return jnp.where(row8 == 0, high, jnp.where(row8 == 1, ssq - high, 0.0)).astype(BF)


def add_y_kernel(got_ref, out_ref):
    tiles = got_ref.shape[1]
    pieces = (tiles - 1) // ZS

    def summed(rows):
        acc = got_ref[0, rows].astype(F32)
        for y in range(1, YS):
            acc = acc + got_ref[y, rows].astype(F32)
        return acc

    tail = split_tail(summed(slice(tiles - 1, tiles))[0])
    for z in range(ZS):
        out_ref[z, :pieces] = summed(slice(z * pieces, (z + 1) * pieces)).astype(BF)
        out_ref[z, pieces] = tail


def make_finish_kernel(inner, last):
    def finish_kernel(got_ref, stream_ref, out_ref):
        tiles = got_ref.shape[1]
        tokens = got_ref.shape[3]
        acc = got_ref[0].astype(F32)
        for z in range(1, ZS):
            acc = acc + got_ref[z].astype(F32)
        ssq = acc[tiles - 1, 0:1] + acc[tiles - 1, 1:2]
        scale = lax.rsqrt(ssq / inner + EPS)
        for j in range(tiles - 1):
            lanes = slice(j * tokens, (j + 1) * tokens)
            new = (stream_ref[:, lanes].astype(F32) + acc[j] * scale).astype(BF)
            if last:
                out_ref[j] = new
            else:
                out_ref[:, lanes] = new

    return finish_kernel


def call(kernel, out_shape, count):
    return pl.pallas_call(
        kernel,
        out_shape=out_shape,
        in_specs=[VMEM] * count,
        out_specs=jax.tree.map(lambda _: VMEM, out_shape),
        compiler_params=limit(10),
    )


def local(
    draft_ids,
    accepted,
    embedding,
    norm_gain,
    w_zx,
    w_dt,
    w_bc,
    dt_bias,
    decay_rate,
    skip_weight,
    conv_x_w,
    conv_x_b,
    conv_bc_w,
    conv_bc_b,
    gate_gain,
    out_w,
    ssm_state,
    conv_x_state,
    conv_bc_state,
):
    seqs, draft = draft_ids.shape
    tokens = seqs * draft
    own_cols = embedding.shape[1]
    model = own_cols * YS * ZS * CS
    width = w_zx.shape[3] // 2
    inner = width * YS * ZS * CS
    bc_here = w_bc.shape[2]
    taps = conv_x_w.shape[1]
    kept = taps - 1
    pieces = own_cols // 8
    states = ssm_state.shape[4]

    tokens_ids = draft_ids.T
    state_shape = (LAYERS, seqs, width, states)

    w_rows = jnp.swapaxes(w_bc, 1, 2)
    row_shape = jax.ShapeDtypeStruct((8, model + 3 * LANES), BF)
    keep, send, table, own8, before_x, before_bc, spread_acc = pl.pallas_call(
        setup_kernel,
        out_shape=(
            row_shape,
            row_shape,
            jax.ShapeDtypeStruct((LAYERS, LANES, LANES), F32),
            jax.ShapeDtypeStruct((LAYERS, 8, model), BF),
            jax.ShapeDtypeStruct((LAYERS, width, tokens), BF),
            jax.ShapeDtypeStruct((LAYERS, 8, tokens), BF),
            jax.ShapeDtypeStruct((8, tokens), jnp.int32),
        ),
        in_specs=[SMEM] * 3 + [VMEM] * 11,
        out_specs=(VMEM,) * 7,
        scratch_shapes=[pltpu.VMEM((LANES, LANES), F32)],
        compiler_params=limit(60),
        name="setup",
    )(
        *[v.reshape(1, LAYERS) for v in (dt_bias, decay_rate, skip_weight)],
        w_rows,
        w_dt.reshape(LAYERS, model),
        jnp.transpose(conv_bc_state, (0, 2, 3, 1)),
        conv_bc_w,
        conv_bc_b,
        norm_gain,
        conv_x_w,
        conv_x_b,
        gate_gain,
        jnp.swapaxes(conv_x_state, 1, 2),
        accepted.reshape(1, seqs),
    )
    pair_rows, pair_states = call(
        pair_kernel,
        (
            jax.ShapeDtypeStruct((8, model + LANES), BF),
            jax.ShapeDtypeStruct((8, 2 * LANES), BF),
        ),
        2,
    )(keep, swap_cores(send))
    pair_rows = pair_rows[None]
    near = join(
        [fetch(pair_rows, lambda x, y, z, c, j=j: (x, y, z + 2 * x + j, c)) for j in range(2)]
    )
    stream = lookup(tokens_ids, embedding.T, pair_states)
    plane = join(
        [near] + [fetch(near, lambda x, y, z, c, d=d: (x, y + d, z, c)) for d in range(1, YS)]
    )
    stream, plane = lax.optimization_barrier((stream, plane))
    w_own = [plane]
    for d in range(1, XS):
        w_own.append(fetch(plane, lambda x, y, z, c, d=d: ((x + d) % XS, y, z, c)))
    own, oth = gather_planes(stream)
    w_oth = [swap_cores(w) for w in w_own]
    first_own, first_oth = own, oth

    tables = [table, own8, before_x, before_bc, spread_acc] + [
        pltpu.with_memory_space_constraint(v, pltpu.HBM)
        for v in (w_zx.reshape(LAYERS, model, 2 * width), out_w, ssm_state.reshape(state_shape))
    ]
    table_specs = [VMEM] * 5 + [HBM] * 3
    saved = ()
    tiles = ZS * pieces + 1
    for layer in range(LAYERS):
        last = layer + 1 == LAYERS
        lead = (LAYERS,) if last else ()
        args = [own, oth, first_own, first_oth, *w_own, *w_oth, *tables, *saved]
        specs = [VMEM] * (4 + 2 * XS) + table_specs + [VMEM, VMEM, HBM][: len(saved)]
        keep, send, *saved = pl.pallas_call(
            make_layer_kernel(layer, tokens, seqs, draft, own_cols, taps, last),
            out_shape=(
                jax.ShapeDtypeStruct((YS, tiles, 8, tokens), F32),
                jax.ShapeDtypeStruct((YS, tiles, 8, tokens), BF),
                jax.ShapeDtypeStruct((*lead, kept, seqs, width), BF),
                jax.ShapeDtypeStruct((*lead, kept, bc_here, seqs), BF),
                jax.ShapeDtypeStruct(state_shape, F32),
            ),
            in_specs=specs,
            out_specs=(VMEM, VMEM, VMEM, VMEM, HBM),
            scratch_shapes=[
                pltpu.VMEM((model, tokens), F32),
                pltpu.VMEM((model, tokens), BF),
                pltpu.VMEM((YS * ZS, 8, model + LANES), BF),
                pltpu.VMEM(state_shape[1:], F32),
                pltpu.VMEM(state_shape[1:], F32),
                pltpu.VMEM((width, tokens), BF),
                pltpu.VMEM((model, 2 * width), BF),
                pltpu.VMEM((width, model), BF),
                pltpu.SemaphoreType.DMA((4,)),
            ],
            input_output_aliases={len(args) - 1: 4} if last else {},
            compiler_params=limit(34),
        )(*args)
        summed = call(
            add_cores_kernel, jax.ShapeDtypeStruct((YS, tiles, 8, tokens), BF), 2
        )(keep, swap_cores(send))
        summed = call(
            add_y_kernel, jax.ShapeDtypeStruct((ZS, pieces + 1, 8, tokens), BF), 1
        )(exchange(summed, Y_GROUPS))
        shape = (pieces, 8, tokens) if last else (8, pieces * tokens)
        stream = call(
            make_finish_kernel(inner, last), jax.ShapeDtypeStruct(shape, BF), 2
        )(exchange(summed, Z_GROUPS), stream)
        if not last:
            own, oth = gather_planes(stream)
    new_x, new_bc, new_ssm = saved
    hidden = stream.reshape(own_cols, tokens).T
    kept_x = jnp.swapaxes(new_x, 1, 2)
    kept_bc = jnp.transpose(new_bc, (0, 3, 1, 2))
    return (hidden, new_ssm.reshape(ssm_state.shape), kept_x, kept_bc)


def solution(mesh):
    placed = (
        P("batch", None),
        P("batch"),
        P(None, "heads"),
        P(),
        P(None, None, "heads", None),
        P(None, None, "heads"),
        P(None, None, "heads"),
        P(None, "heads"),
        P(None, "heads"),
        P(None, "heads"),
        P(None, None, "heads"),
        P(None, "heads"),
        P(None, None, "heads"),
        P(None, "heads"),
        P(None, "heads"),
        P(None, "heads", None),
        P(None, "batch", "heads", None, None),
        P(None, "batch", None, "heads"),
        P(None, "batch", None, "heads"),
    )
    return jax.shard_map(
        local,
        mesh=mesh,
        in_specs=placed,
        out_specs=(
            P("batch", "heads"),
            P(None, "batch", "heads", None, None),
            P(None, "batch", None, "heads"),
            P(None, "batch", None, "heads"),
        ),
        check_vma=False,
    )
```

```python
import jax
import jax.numpy as jnp
from jax import lax
from jax.experimental import pallas as pl
from jax.experimental.pallas import tpu as pltpu
from jax.sharding import PartitionSpec as P


LAYERS = 2
EPS = 1e-05
BF = jnp.bfloat16
F32 = jnp.float32
LANES = 128

YS, ZS, CS = 4, 8, 2


def device_at(y, z, c):
    return (y * ZS + z) * CS + c


Z_GROUPS = [[device_at(y, z, c) for z in range(ZS)] for y in range(YS) for c in range(CS)]
Y_GROUPS = [[device_at(y, z, c) for y in range(YS)] for z in range(ZS) for c in range(CS)]
PARTNER = [(i, i ^ 1) for i in range(YS * ZS * CS)]


PLACES = [(y, z, c) for y in range(YS) for z in range(ZS) for c in range(CS)]


def from_y(value, shift):
    pairs = [(device_at((y + shift) % YS, z, c), device_at(y, z, c)) for y, z, c in PLACES]
    return lax.ppermute(value, "heads", pairs)


def swap_cores(value):
    return lax.ppermute(value, "heads", PARTNER)


def exchange(value, groups):
    return lax.all_to_all(value, "heads", 0, 0, tiled=True, axis_index_groups=groups)


def spread(value, groups):
    count = len(groups[0])
    return exchange(jnp.broadcast_to(value[None], (count, *value.shape)), groups)


def gather_planes(piece, ring):
    rows, width = piece.shape
    half = ZS // 2
    over_z = spread(piece, Z_GROUPS)
    if ring:
        below = from_y(over_z, -1)
        above = from_y(over_z, 1)
        far_low = from_y(below[:half], -1)
        far_high = from_y(above[half:], 1)
        own = call(
            ring_join_kernel, jax.ShapeDtypeStruct((YS * ZS, rows, width), BF), 5
        )(over_z, below, above, far_low, far_high)
    else:
        own = spread(over_z, Y_GROUPS).reshape(YS * ZS, rows, width)
    return own, swap_cores(own)


def ring_join_kernel(here_ref, below_ref, above_ref, low_ref, high_ref, out_ref):
    y = position()[0]
    half = ZS // 2
    for shift, ref in ((0, here_ref), (1, above_ref), (3, below_ref)):
        out_ref[pl.ds(lax.rem(y + shift, YS) * ZS, ZS)] = ref[...]
    far = lax.rem(y + 2, YS) * ZS
    out_ref[pl.ds(far, half)] = low_ref[...]
    out_ref[pl.ds(far + half, half)] = high_ref[...]


VMEM = pl.BlockSpec(memory_space=pltpu.VMEM)
SMEM = pl.BlockSpec(memory_space=pltpu.SMEM)
HBM = pl.BlockSpec(memory_space=pltpu.HBM)


def limit(mib):
    return pltpu.CompilerParams(vmem_limit_bytes=mib * 1024 * 1024)


def silu(v):
    return v / (1.0 + jnp.exp(-v))


def softplus(v):
    e = jnp.exp(-jnp.abs(v))
    grown = 1.0 + e
    small = grown == 1.0
    log1p = jnp.where(small, e, jnp.log(grown) * (e / jnp.where(small, 1.0, grown - 1.0)))
    return jnp.maximum(v, 0.0) + log1p


SHIFT = LANES.bit_length() - 1


def position():
    at = lax.axis_index("heads")
    return at // (ZS * CS), at // CS % ZS, at % CS


def lookup_kernel(ids_ref, table_ref, out_ref, tail_ref, acc_ref):
    rows, vocab = table_ref.shape
    draft = ids_ref.shape[0]
    tokens = acc_ref.shape[1]
    whole = vocab // LANES
    tail_at = whole * LANES
    lane = lax.broadcasted_iota(jnp.int32, (rows, LANES), 1)
    tail_ref[...] = jnp.zeros_like(tail_ref)
    if tail_at < vocab:
        tail_ref[:, : vocab - tail_at] = table_ref[:, tail_at:].astype(F32)
    tail = tail_ref[...]
    seqs_a_tile = LANES // draft
    for tile in range(tokens // LANES):

        def one(s, acc, tile=tile):
            for t in range(draft):
                token = ids_ref[t, tile * seqs_a_tile + s]
                i = s * draft + t
                block = jnp.minimum(token >> SHIFT, whole - 1)
                at = pl.multiple_of(block << SHIFT, LANES)
                found = table_ref[:, pl.ds(at, LANES)].astype(F32)
                found = jnp.where(token >= tail_at, tail, found)
                moved = pltpu.roll(found, (i - token) & (LANES - 1), 1)
                acc = jnp.where(lane == i, moved, acc)
            return acc

        acc = lax.fori_loop(0, seqs_a_tile, one, jnp.zeros((rows, LANES), F32), unroll=2)
        acc_ref[:, tile * LANES : (tile + 1) * LANES] = acc
    for j in range(rows // 8):
        out_ref[:, j * tokens : (j + 1) * tokens] = acc_ref[8 * j : 8 * j + 8, :].astype(BF)


def lookup(ids, table):
    rows = table.shape[0]
    tokens = ids.size
    return pl.pallas_call(
        lookup_kernel,
        out_shape=jax.ShapeDtypeStruct((8, rows // 8 * tokens), BF),
        in_specs=[SMEM, VMEM],
        out_specs=VMEM,
        scratch_shapes=[pltpu.VMEM((rows, LANES), F32), pltpu.VMEM((rows, tokens), F32)],
        compiler_params=limit(12),
        name="lookup",
    )(ids, table)


def tdot(a, b):
    return lax.dot_general(a, b, (((0,), (0,)), ((), ())), preferred_element_type=F32)


def ndot(a, b):
    return lax.dot_general(a, b, (((1,), (1,)), ((), ())), preferred_element_type=F32)


def mdot(a, b):
    return lax.dot_general(a, b, (((1,), (0,)), ((), ())), preferred_element_type=F32)


SLOT = 64
AT_TAPS, AT_ACCEPTED, AT_BIAS, AT_RATE, AT_SKIP = 24, 32, 33, 34, 35


def saved_at(j, kept, seqs, draft):
    seq = lax.broadcasted_iota(jnp.int32, (seqs, seqs * draft), 0)
    at = lax.broadcasted_iota(jnp.int32, (seqs, seqs * draft), 1)
    return (at == seq * draft + (draft - kept) + j).astype(F32).astype(BF)


def setup_kernel(
    bias_ref, rate_ref, skip_ref, w_ref, wdt_ref, state_ref, taps_ref, tapb_ref, gain_ref,
    xtaps_ref, xtapb_ref, gate_ref, statex_ref, accepted_ref,
    vocab_ref,
    keep_ref, send_ref, table_ref, own8_ref, beforex_ref, beforebc_ref, spread_ref, near_ref,
    table, sem,
):
    bring = pltpu.make_async_copy(vocab_ref, near_ref, sem)
    bring.start()
    model = w_ref.shape[2]
    here = w_ref.shape[1]
    kept, seqs = state_ref.shape[1], state_ref.shape[3]
    draft = spread_ref.shape[1] // seqs
    taps = taps_ref.shape[1]
    width = xtaps_ref.shape[2]
    first = position()[2] == 0
    places = [saved_at(j, kept, seqs, draft) for j in range(kept)]
    outs, rows = [], []
    for layer in range(LAYERS):
        table[...] = jnp.zeros_like(table)
        table[0:taps, 0:here] = taps_ref[layer].astype(F32)
        table[taps : taps + 1, 0:here] = tapb_ref[layer : layer + 1].astype(F32)
        turned = jnp.transpose(table[...])[:8]
        tiles = []
        for j in range(kept):
            table[...] = jnp.zeros_like(table)
            table[0:here, 0:seqs] = state_ref[layer, j].astype(F32)
            tiles.append(table[0:8, :])
        outs.append((turned, tiles[0] + pltpu.roll(tiles[1], SLOT, 1), tiles[2]))
        row = w_ref[layer].astype(F32)
        rows.append(jnp.concatenate([row, jnp.zeros((8 - here, model), F32)], axis=0))
        own8_ref[layer] = jnp.concatenate(
            [row, wdt_ref[layer : layer + 1, :].astype(F32), jnp.zeros((7 - here, model), F32)], axis=0
        ).astype(BF)
    for ref, pick in ((keep_ref, first), (send_ref, jnp.logical_not(first))):
        for lo, values in (
            (0, rows),
            (model, [o[0] for o in outs]),
            (model + LANES, [o[1] for o in outs]),
            (model + 2 * LANES, [o[2] for o in outs]),
        ):
            value = jnp.where(pick, values[0], values[1])
            value = jnp.where(first, value, pltpu.roll(value, here, 0))
            ref[:, lo : lo + value.shape[1]] = value.astype(BF)
    for layer in range(LAYERS):
        table[...] = jnp.zeros_like(table)
        for j in range(model // LANES):
            table[j : j + 1, :] = gain_ref[layer : layer + 1, j * LANES : (j + 1) * LANES]
        table[AT_TAPS : AT_TAPS + taps, :width] = xtaps_ref[layer].astype(F32)
        table[AT_TAPS + taps : AT_TAPS + taps + 1, :width] = xtapb_ref[layer : layer + 1].astype(F32)
        table[AT_TAPS + taps + 1 : AT_TAPS + taps + 2, :width] = gate_ref[layer : layer + 1]
        table[AT_ACCEPTED : AT_ACCEPTED + 1, :seqs] = accepted_ref[...].astype(F32)
        table[AT_BIAS : AT_BIAS + 1, :] = jnp.broadcast_to(bias_ref[0:1, layer : layer + 1], (1, LANES))
        table[AT_RATE : AT_RATE + 1, :] = jnp.broadcast_to(rate_ref[0:1, layer : layer + 1], (1, LANES))
        table[AT_SKIP : AT_SKIP + 1, :] = jnp.broadcast_to(skip_ref[0:1, layer : layer + 1], (1, LANES))
        table_ref[layer] = jnp.transpose(table[...])
        beforex_ref[layer] = sum(tdot(statex_ref[layer, j], places[j]) for j in range(kept)).astype(BF)
        beforebc_ref[layer] = jnp.concatenate(
            [
                sum(mdot(state_ref[layer, j], places[j]) for j in range(kept)),
                jnp.zeros((8 - here, seqs * draft), F32),
            ],
            axis=0,
        ).astype(BF)
    seq = lax.broadcasted_iota(jnp.int32, (seqs, seqs * draft), 0)
    at = lax.broadcasted_iota(jnp.int32, (seqs, seqs * draft), 1)
    owner = (at // draft == seq).astype(F32).astype(BF)
    spread_ref[...] = mdot(
        jnp.broadcast_to(accepted_ref[...].astype(F32), (8, seqs)).astype(BF), owner
    ).astype(jnp.int32)
    bring.wait()


def pair_kernel(keep_ref, got_ref, rows_ref):
    rows_ref[...] = (keep_ref[...].astype(F32) + got_ref[...].astype(F32)).astype(BF)


def convolve(now, before, weights, bias, draft):
    tokens = now.shape[1]
    taps = len(weights)
    t0 = lax.broadcasted_iota(jnp.int32, (1, tokens), 1) % draft
    acc = None
    for k in range(taps):
        d = taps - 1 - k
        shifted = now
        if d:
            shifted = jnp.where(
                t0 >= d, pltpu.roll(now, d, 1), pltpu.roll(before, tokens - (draft - d), 1)
            )
        term = shifted * weights[k]
        acc = term if acc is None else acc + term
    return silu(acc + bias)


def make_project_kernel(layer, tokens, seqs, draft, own_cols, taps):
    model = own_cols * YS * ZS * CS
    pieces = own_cols // 8
    kept = taps - 1

    def kernel(
        own_ref, oth_ref, wown_ref, woth_ref, table_ref, own8_ref, nb_ref, mine_ref, bcc_ref, xs
    ):
        core = position()[2]
        first = core == 0
        turned = table_ref[layer]

        total = jnp.zeros((8, tokens), F32)
        for k in range(YS * ZS):
            for j in range(pieces):
                lanes = slice(j * tokens, (j + 1) * tokens)
                a = own_ref[k, :, lanes].astype(F32)
                b = oth_ref[k, :, lanes].astype(F32)
                total = total + a * a + b * b
                at = 2 * k * own_cols + 8 * j
                xs[at : at + 8, :] = jnp.where(first, a, b)
                xs[at + own_cols : at + own_cols + 8, :] = jnp.where(first, b, a)
        scale = lax.rsqrt(jnp.sum(total, axis=0, keepdims=True) / model + EPS)
        for j in range(model // LANES):
            at = slice(j * LANES, (j + 1) * LANES)
            nb_ref[at, :] = ((xs[at, :] * scale) * turned[:, j : j + 1]).astype(BF)

        take_own = core == layer
        count = ZS * 8
        rows = jnp.where(take_own, wown_ref[...].astype(F32), woth_ref[...].astype(F32)).reshape(
            count, model + 3 * LANES
        )
        left = jnp.concatenate([rows[:, :model], own8_ref[layer].astype(F32)], axis=0).astype(BF)
        out = mdot(left, nb_ref[...]).astype(BF)
        mine_ref[...] = out[count:]
        slot = lax.broadcasted_iota(jnp.int32, (2 * LANES, tokens), 0)
        slot_lane = lax.broadcasted_iota(jnp.int32, (2 * LANES, tokens), 1)
        slot_seq, slot_j = slot & (SLOT - 1), slot // SLOT
        place = (
            (slot_seq < seqs) & (slot_j < kept) & (slot_lane == slot_seq * draft + (draft - kept) + slot_j)
        ).astype(F32).astype(BF)
        before = mdot(rows[:, model + LANES :].astype(BF), place)
        extra = rows[:, model : model + LANES]
        bcc = convolve(
            out[:count].astype(F32),
            before,
            [extra[:, k : k + 1] for k in range(taps)],
            extra[:, taps : taps + 1],
            draft,
        )
        bcc_ref[...] = bcc.astype(BF)

    return kernel


def make_values_kernel(layer, tokens, seqs, draft, taps, last):
    kept = taps - 1

    def kernel(*refs):
        (
            nb_ref, mine_ref, table_ref, beforex_ref, beforebc_ref, spread_ref, zx_ref, *rest,
        ) = refs
        if last:
            old_x_ref, old_bc_ref, *rest = rest
        gate_ref, xc_ref, rows_ref, newx_ref, newbc_ref, zx_w, sem = rest
        load_w = pltpu.make_async_copy(zx_ref.at[layer], zx_w, sem)
        load_w.start()
        turned = table_ref[layer]
        width = beforex_ref.shape[1]
        here = newbc_ref.shape[-2]
        acc_col = turned[:seqs, AT_ACCEPTED : AT_ACCEPTED + 1].astype(jnp.int32)
        cols = turned[:width, AT_TAPS : AT_TAPS + 8]
        bias_dt = turned[:1, AT_BIAS : AT_BIAS + 1]
        rate = turned[:1, AT_RATE : AT_RATE + 1]
        lane = lax.broadcasted_iota(jnp.int32, (1, tokens), 1)
        t0 = lane % draft
        mine = mine_ref[...]
        before_b, before_mb = beforex_ref[layer], beforebc_ref[layer]

        step = softplus(mine[here : here + 1, :].astype(F32) + bias_dt)
        cum = step
        for d in (1, 2, 4):
            cum = cum + jnp.where(t0 >= d, pltpu.roll(cum, d, 1), 0.0)
        accepted = spread_ref[:1]
        cut = jnp.where(t0 < accepted, step, 0.0)
        for d in (1, 2, 4):
            cut = cut + jnp.where((t0 & d) != 0, pltpu.roll(cut, d, 1), pltpu.roll(cut, tokens - d, 1))
        weight = jnp.where(t0 < accepted, jnp.exp(-rate * (cut - cum)) * step, 0.0)
        rows = (step, cum, jnp.exp(-rate * cum), jnp.exp(-rate * cut), weight)
        for i, row in enumerate(rows):
            rows_ref[i : i + 1, :] = row
        rows_ref[len(rows) :, :] = jnp.zeros((8 - len(rows), tokens), F32)

        load_w.wait()
        zx = tdot(zx_w[...], nb_ref[...]).astype(BF)
        gate_ref[...] = silu(zx[:width].astype(F32))
        values_b = zx[width:]
        xc_ref[...] = convolve(
            values_b.astype(F32),
            before_b.astype(F32),
            [cols[:, k : k + 1] for k in range(taps)],
            cols[:, taps : taps + 1],
            draft,
        )

        seq = lax.broadcasted_iota(jnp.int32, (seqs, tokens), 0)
        at = lax.broadcasted_iota(jnp.int32, (seqs, tokens), 1)
        for i in range(kept):
            row = acc_col + i
            new = ((at == seq * draft + row - kept) & (row >= kept)).astype(F32).astype(BF)
            old = ((at == seq * draft + (draft - kept) + row) & (row < kept)).astype(F32).astype(BF)
            rows_x = (ndot(new, values_b) + ndot(old, before_b)).astype(BF)
            rows_bc = (ndot(mine, new) + ndot(before_mb, old))[:here].astype(BF)
            if last:
                newx_ref[layer, i], newbc_ref[layer, i] = rows_x, rows_bc
                for l in range(layer):
                    newx_ref[l, i], newbc_ref[l, i] = old_x_ref[i], old_bc_ref[i]
            else:
                newx_ref[i], newbc_ref[i] = rows_x, rows_bc

    return kernel


def make_recur_kernel(layer, tokens, draft, own_cols, taps, last):
    pieces = own_cols // 8

    def kernel(*refs):
        got_refs = refs[:YS]
        gate_ref, xc_ref, rows_ref, table_ref, outw_ref, ssm_ref, *rest = refs[YS:]
        if last:
            _, *rest = rest
        keep_ref, send_ref, newssm_ref, h_in, h_out, xw_all, out_w, channels, sems = rest
        y_here, _, core = position()
        first = core == 0
        tiles = xc_ref.shape[1] // LANES
        part = h_in.shape[0] // tiles
        loads = []
        for i in range(tiles):
            at = pl.ds(i * part, part)
            loads.append(pltpu.make_async_copy(ssm_ref.at[layer, at], h_in.at[at], sems.at[i]))
            loads[-1].start()
        load_o = pltpu.make_async_copy(outw_ref.at[layer], out_w, sems.at[tiles])
        load_o.start()
        turned = table_ref[layer]
        width = xc_ref.shape[0]
        rate = turned[:1, AT_RATE : AT_RATE + 1]
        skip = turned[:1, AT_SKIP : AT_SKIP + 1]
        gain = turned[:width, AT_TAPS + taps + 1 : AT_TAPS + taps + 2]
        xc = xc_ref[...]
        step, cum, fall, fall_cut, weight = [rows_ref[i : i + 1, :] for i in range(5)]
        for d, ref in enumerate(got_refs):
            channels[lax.rem(y_here + d, YS)] = ref[...].astype(F32)
        bcc = channels[...].reshape(-1, xc_ref.shape[1]).astype(BF)
        states = bcc.shape[0] // 2
        xb = xc.astype(BF)
        xw_all[...] = (xc * weight).astype(BF)

        per_tile = LANES // draft
        sub = lax.broadcasted_iota(jnp.int32, (LANES, LANES), 0)
        lan = lax.broadcasted_iota(jnp.int32, (LANES, LANES), 1)
        causal = (sub // draft == lan // draft) & (sub <= lan)
        group = lax.broadcasted_iota(jnp.int32, (1, LANES), 1) // draft
        pick16 = lax.broadcasted_iota(jnp.int32, (per_tile, LANES), 0) * draft == (
            lax.broadcasted_iota(jnp.int32, (per_tile, LANES), 1)
        )
        parts = []
        for tile in range(tokens // LANES):
            ls = slice(tile * LANES, (tile + 1) * LANES)
            bmat = bcc[:states, ls]
            cmat = bcc[states:, ls]
            cum_r = jnp.broadcast_to(cum[:, ls], (LANES, LANES))
            step_c = jnp.transpose(jnp.broadcast_to(step[:, ls], (LANES, LANES)))
            cum_c = jnp.transpose(cum_r)
            gram = tdot(bmat, cmat)
            within = jnp.where(causal, gram * (jnp.exp(-rate * (cum_r - cum_c)) * step_c), 0.0)
            y_new = mdot(xb[:, ls], within.astype(BF))
            y_old = jnp.zeros((width, LANES), F32)
            falls = jnp.sum(jnp.where(pick16, fall_cut[:, ls], 0.0), axis=1, keepdims=True)
            xw = xw_all[:, ls]
            loads[tile].wait()
            for s in range(per_tile):
                n = tile * per_tile + s
                h0 = h_in[n]
                here = group == s
                y_old = jnp.where(here, mdot(h0.astype(BF), cmat), y_old)
                add = ndot(jnp.where(here, xw, jnp.zeros_like(xw)), bmat)
                h_out[n] = h0 * falls[s : s + 1, :] + add
            parts.append(fall[:, ls] * y_old + y_new)
        store = pltpu.make_async_copy(h_out, newssm_ref.at[layer], sems.at[tiles + 1])
        store.start()
        y = jnp.concatenate(parts, axis=1) + skip * xc
        gated = y * gate_ref[...]
        ssq = jnp.sum(gated * gated, axis=0, keepdims=True)
        u = (gated * gain).astype(BF)

        high = ssq.astype(BF)
        low = (ssq - high.astype(F32)).astype(BF)
        row8 = lax.broadcasted_iota(jnp.int32, (8, tokens), 0)
        tail = jnp.where(row8 == 0, high.astype(F32), jnp.where(row8 == 1, low.astype(F32), 0.0))
        block = own_cols * CS * ZS
        load_o.wait()
        for y_at in range(YS):
            out = tdot(out_w[:, y_at * block : (y_at + 1) * block], u)
            out = out.reshape(ZS, CS, pieces, 8, tokens)
            for z in range(ZS):
                even, odd = out[z, 0], out[z, 1]
                rows = slice(z * pieces, (z + 1) * pieces)
                keep_ref[y_at, rows] = jnp.where(first, even, odd)
                send_ref[y_at, rows] = jnp.where(first, odd, even).astype(BF)
            keep_ref[y_at, ZS * pieces] = tail
            send_ref[y_at, ZS * pieces] = tail.astype(BF)
        store.wait()

    return kernel


def add_cores_kernel(keep_ref, got_ref, *out_refs):
    tiles = keep_ref.shape[1]
    y = position()[0]
    tail = split_tail(keep_ref[0, tiles - 1] + got_ref[0, tiles - 1].astype(F32))
    for shift, out_ref in enumerate(out_refs):
        at = lax.rem(y + shift, YS)
        out_ref[: tiles - 1] = (
            keep_ref[at, : tiles - 1] + got_ref[at, : tiles - 1].astype(F32)
        ).astype(BF)
        out_ref[tiles - 1] = tail


def split_tail(tail):
    row8 = lax.broadcasted_iota(jnp.int32, tail.shape, 0)
    ssq = tail[0:1] + tail[1:2]
    high = ssq.astype(BF).astype(F32)
    return jnp.where(row8 == 0, high, jnp.where(row8 == 1, ssq - high, 0.0)).astype(BF)


def add_y_kernel(*refs):
    *got_refs, out_ref = refs
    tiles = got_refs[0].shape[0]
    pieces = (tiles - 1) // ZS

    def summed(rows):
        acc = got_refs[0][rows].astype(F32)
        for ref in got_refs[1:]:
            acc = acc + ref[rows].astype(F32)
        return acc

    tail = split_tail(summed(slice(tiles - 1, tiles))[0])
    for z in range(ZS):
        out_ref[z, :pieces] = summed(slice(z * pieces, (z + 1) * pieces)).astype(BF)
        out_ref[z, pieces] = tail


def make_finish_kernel(inner, last):
    def finish_kernel(got_ref, stream_ref, out_ref):
        tiles = got_ref.shape[1]
        tokens = got_ref.shape[3]
        acc = got_ref[0].astype(F32)
        for z in range(1, ZS):
            acc = acc + got_ref[z].astype(F32)
        ssq = acc[tiles - 1, 0:1] + acc[tiles - 1, 1:2]
        scale = lax.rsqrt(ssq / inner + EPS)
        for j in range(tiles - 1):
            lanes = slice(j * tokens, (j + 1) * tokens)
            new = (stream_ref[:, lanes].astype(F32) + acc[j] * scale).astype(BF)
            if last:
                out_ref[j] = new
            else:
                out_ref[:, lanes] = new

    return finish_kernel


def call(kernel, out_shape, count):
    return pl.pallas_call(
        kernel,
        out_shape=out_shape,
        in_specs=[VMEM] * count,
        out_specs=jax.tree.map(lambda _: VMEM, out_shape),
        compiler_params=limit(10),
    )


def local(
    draft_ids,
    accepted,
    embedding,
    norm_gain,
    w_zx,
    w_dt,
    w_bc,
    dt_bias,
    decay_rate,
    skip_weight,
    conv_x_w,
    conv_x_b,
    conv_bc_w,
    conv_bc_b,
    gate_gain,
    out_w,
    ssm_state,
    conv_x_state,
    conv_bc_state,
):
    seqs, draft = draft_ids.shape
    tokens = seqs * draft
    own_cols = embedding.shape[1]
    model = own_cols * YS * ZS * CS
    width = w_zx.shape[3] // 2
    inner = width * YS * ZS * CS
    bc_here = w_bc.shape[2]
    taps = conv_x_w.shape[1]
    kept = taps - 1
    pieces = own_cols // 8
    states = ssm_state.shape[4]

    tokens_ids = draft_ids.T
    state_shape = (LAYERS, seqs, width, states)

    w_rows = jnp.swapaxes(w_bc, 1, 2)
    row_shape = jax.ShapeDtypeStruct((8, model + 3 * LANES), BF)
    keep, send, table, own8, before_x, before_bc, spread_acc, vocab = pl.pallas_call(
        setup_kernel,
        out_shape=(
            row_shape,
            row_shape,
            jax.ShapeDtypeStruct((LAYERS, LANES, LANES), F32),
            jax.ShapeDtypeStruct((LAYERS, 8, model), BF),
            jax.ShapeDtypeStruct((LAYERS, width, tokens), BF),
            jax.ShapeDtypeStruct((LAYERS, 8, tokens), BF),
            jax.ShapeDtypeStruct((8, tokens), jnp.int32),
            jax.ShapeDtypeStruct(embedding.shape[::-1], BF),
        ),
        in_specs=[VMEM] * 14 + [HBM],
        out_specs=(VMEM,) * 8,
        scratch_shapes=[pltpu.VMEM((LANES, LANES), F32), pltpu.SemaphoreType.DMA],
        compiler_params=limit(16),
        name="setup",
    )(
        *[
            pltpu.with_memory_space_constraint(v, pltpu.HBM)
            for v in (
                *[v.reshape(1, LAYERS) for v in (dt_bias, decay_rate, skip_weight)],
                w_rows,
                w_dt.reshape(LAYERS, model),
                jnp.transpose(conv_bc_state, (0, 2, 3, 1)),
                conv_bc_w,
                conv_bc_b,
                norm_gain,
                conv_x_w,
                conv_x_b,
                gate_gain,
                jnp.swapaxes(conv_x_state, 1, 2),
                accepted.reshape(1, seqs),
                embedding.T,
            )
        ],
    )
    pair_rows = call(pair_kernel, row_shape, 2)(keep, swap_cores(send))
    stream = lookup(tokens_ids, vocab)
    w_own = spread(pair_rows, Z_GROUPS)
    w_oth = swap_cores(w_own)
    own, oth = gather_planes(stream, True)

    zx_w, outer_w, state_in = [
        pltpu.with_memory_space_constraint(v, pltpu.HBM)
        for v in (w_zx.reshape(LAYERS, model, 2 * width), out_w, ssm_state.reshape(state_shape))
    ]
    saved, saved_ssm = (), ()
    tiles = ZS * pieces + 1
    for layer in range(LAYERS):
        last = layer + 1 == LAYERS
        lead = (LAYERS,) if last else ()
        normed, mine, bcc = pl.pallas_call(
            make_project_kernel(layer, tokens, seqs, draft, own_cols, taps),
            out_shape=(
                jax.ShapeDtypeStruct((model, tokens), BF),
                jax.ShapeDtypeStruct((8, tokens), BF),
                jax.ShapeDtypeStruct((ZS * 8, tokens), BF),
            ),
            in_specs=[VMEM] * 6,
            out_specs=(VMEM,) * 3,
            scratch_shapes=[pltpu.VMEM((model, tokens), F32)],
            compiler_params=limit(20),
        )(own, oth, w_own, w_oth, table, own8)
        got = [bcc] + [from_y(bcc, d) for d in range(1, YS)]
        gate, xc, rows, *saved = pl.pallas_call(
            make_values_kernel(layer, tokens, seqs, draft, taps, last),
            out_shape=(
                jax.ShapeDtypeStruct((width, tokens), F32),
                jax.ShapeDtypeStruct((width, tokens), F32),
                jax.ShapeDtypeStruct((8, tokens), F32),
                jax.ShapeDtypeStruct((*lead, kept, seqs, width), BF),
                jax.ShapeDtypeStruct((*lead, kept, bc_here, seqs), BF),
            ),
            in_specs=[VMEM] * 6 + [HBM] + [VMEM] * len(saved),
            out_specs=(VMEM,) * 5,
            scratch_shapes=[
                pltpu.VMEM((model, 2 * width), BF),
                pltpu.SemaphoreType.DMA,
            ],
            compiler_params=limit(16),
            cost_estimate=pl.CostEstimate(
                flops=2 * model * tokens * 4 * width, bytes_accessed=4 << 20, transcendentals=0
            ),
        )(
            normed, mine, table, before_x, before_bc, spread_acc, zx_w, *saved
        )
        keep, send, *saved_ssm = pl.pallas_call(
            make_recur_kernel(layer, tokens, draft, own_cols, taps, last),
            out_shape=(
                jax.ShapeDtypeStruct((YS, tiles, 8, tokens), F32),
                jax.ShapeDtypeStruct((YS, tiles, 8, tokens), BF),
                jax.ShapeDtypeStruct(state_shape, F32),
            ),
            in_specs=[VMEM] * 8 + [HBM] * (2 + len(saved_ssm)),
            out_specs=(VMEM, VMEM, HBM),
            scratch_shapes=[
                pltpu.VMEM(state_shape[1:], F32),
                pltpu.VMEM(state_shape[1:], F32),
                pltpu.VMEM((width, tokens), BF),
                pltpu.VMEM((width, model), BF),
                pltpu.VMEM((YS, ZS * 8, tokens), F32),
                pltpu.SemaphoreType.DMA((tokens // LANES + 2,)),
            ],
            input_output_aliases={10: 2} if last else {},
            compiler_params=limit(24),
        )(*got, gate, xc, rows, table, outer_w, state_in, *saved_ssm)
        block = jax.ShapeDtypeStruct((tiles, 8, tokens), BF)
        here, *blocks = call(add_cores_kernel, (block,) * YS, 2)(keep, swap_cores(send))
        got = {d: from_y(blocks[d - 1], -d) for d in (2, 1, 3)}
        summed = call(
            add_y_kernel, jax.ShapeDtypeStruct((ZS, pieces + 1, 8, tokens), BF), YS
        )(here, *[got[d] for d in range(1, YS)])
        shape = (pieces, 8, tokens) if last else (8, pieces * tokens)
        stream = call(
            make_finish_kernel(inner, last), jax.ShapeDtypeStruct(shape, BF), 2
        )(exchange(summed, Z_GROUPS), stream)
        if not last:
            own, oth = gather_planes(stream, False)
    (new_x, new_bc), (new_ssm,) = saved, saved_ssm
    hidden = stream.reshape(own_cols, tokens).T
    kept_x = jnp.swapaxes(new_x, 1, 2)
    kept_bc = jnp.transpose(new_bc, (0, 3, 1, 2))
    return (hidden, new_ssm.reshape(ssm_state.shape), kept_x, kept_bc)


def solution(mesh):
    placed = (
        P("batch", None),
        P("batch"),
        P(None, "heads"),
        P(),
        P(None, None, "heads", None),
        P(None, None, "heads"),
        P(None, None, "heads"),
        P(None, "heads"),
        P(None, "heads"),
        P(None, "heads"),
        P(None, None, "heads"),
        P(None, "heads"),
        P(None, None, "heads"),
        P(None, "heads"),
        P(None, "heads"),
        P(None, "heads", None),
        P(None, "batch", "heads", None, None),
        P(None, "batch", None, "heads"),
        P(None, "batch", None, "heads"),
    )
    return jax.shard_map(
        local,
        mesh=mesh,
        in_specs=placed,
        out_specs=(
            P("batch", "heads"),
            P(None, "batch", "heads", None, None),
            P(None, "batch", None, "heads"),
            P(None, "batch", None, "heads"),
        ),
        check_vma=False,
    )
```

```python
import jax
import jax.numpy as jnp
from jax import lax
from jax.experimental import pallas as pl
from jax.experimental.pallas import tpu as pltpu
from jax.sharding import PartitionSpec as P


LAYERS = 2
EPS = 1e-05
BF = jnp.bfloat16
F32 = jnp.float32
LANES = 128

YS, ZS, CS = 4, 8, 2


def device_at(y, z, c):
    return (y * ZS + z) * CS + c


Z_GROUPS = [[device_at(y, z, c) for z in range(ZS)] for y in range(YS) for c in range(CS)]
PARTNER = [(i, i ^ 1) for i in range(YS * ZS * CS)]


PLACES = [(y, z, c) for y in range(YS) for z in range(ZS) for c in range(CS)]


def from_y(value, shift):
    pairs = [(device_at((y + shift) % YS, z, c), device_at(y, z, c)) for y, z, c in PLACES]
    return lax.ppermute(value, "heads", pairs)


def to_y(value, shift):
    pairs = [
        (device_at(y, z, c), device_at((y + (shift if c == 0 else -shift)) % YS, z, c))
        for y, z, c in PLACES
    ]
    return lax.ppermute(value, "heads", pairs)


def swap_cores(value):
    return lax.ppermute(value, "heads", PARTNER)


def exchange(value, groups):
    return lax.all_to_all(value, "heads", 0, 0, tiled=True, axis_index_groups=groups)


def spread(value, groups):
    count = len(groups[0])
    return exchange(jnp.broadcast_to(value[None], (count, *value.shape)), groups)


def gather_planes(piece):
    rows, width = piece.shape
    over_z = spread(piece, Z_GROUPS)
    own = call(
        join_y_kernel, jax.ShapeDtypeStruct((YS * ZS, rows, width), BF), YS
    )(over_z, *[to_y(over_z, d) for d in range(1, YS)])
    return own, swap_cores(own)


def join_y_kernel(*refs):
    *got_refs, out_ref = refs
    y, _, core = position()
    turn = jnp.where(core == 0, YS - 1, 1)
    for d, ref in enumerate(got_refs):
        out_ref[pl.ds(lax.rem(y + d * turn, YS) * ZS, ZS)] = ref[...]


VMEM = pl.BlockSpec(memory_space=pltpu.VMEM)
SMEM = pl.BlockSpec(memory_space=pltpu.SMEM)
HBM = pl.BlockSpec(memory_space=pltpu.HBM)


def limit(mib):
    return pltpu.CompilerParams(vmem_limit_bytes=mib * 1024 * 1024)


def silu(v):
    return v / (1.0 + jnp.exp(-v))


def softplus(v):
    e = jnp.exp(-jnp.abs(v))
    grown = 1.0 + e
    small = grown == 1.0
    log1p = jnp.where(small, e, jnp.log(grown) * (e / jnp.where(small, 1.0, grown - 1.0)))
    return jnp.maximum(v, 0.0) + log1p


SHIFT = LANES.bit_length() - 1


def position():
    at = lax.axis_index("heads")
    return at // (ZS * CS), at // CS % ZS, at % CS


def lookup_kernel(ids_ref, table_ref, out_ref, tail_ref, acc_ref):
    rows, vocab = table_ref.shape
    draft = ids_ref.shape[0]
    tokens = acc_ref.shape[1]
    whole = vocab // LANES
    tail_at = whole * LANES
    lane = lax.broadcasted_iota(jnp.int32, (rows, LANES), 1)
    tail_ref[...] = jnp.zeros_like(tail_ref)
    if tail_at < vocab:
        tail_ref[:, : vocab - tail_at] = table_ref[:, tail_at:].astype(F32)
    tail = tail_ref[...]
    seqs_a_tile = LANES // draft
    for tile in range(tokens // LANES):

        def one(s, acc, tile=tile):
            for t in range(draft):
                token = ids_ref[t, tile * seqs_a_tile + s]
                i = s * draft + t
                block = jnp.minimum(token >> SHIFT, whole - 1)
                at = pl.multiple_of(block << SHIFT, LANES)
                found = table_ref[:, pl.ds(at, LANES)].astype(F32)
                found = jnp.where(token >= tail_at, tail, found)
                moved = pltpu.roll(found, (i - token) & (LANES - 1), 1)
                acc = jnp.where(lane == i, moved, acc)
            return acc

        acc = lax.fori_loop(0, seqs_a_tile, one, jnp.zeros((rows, LANES), F32), unroll=2)
        acc_ref[:, tile * LANES : (tile + 1) * LANES] = acc
    for j in range(rows // 8):
        out_ref[:, j * tokens : (j + 1) * tokens] = acc_ref[8 * j : 8 * j + 8, :].astype(BF)


def lookup(ids, table):
    rows = table.shape[0]
    tokens = ids.size
    return pl.pallas_call(
        lookup_kernel,
        out_shape=jax.ShapeDtypeStruct((8, rows // 8 * tokens), BF),
        in_specs=[SMEM, VMEM],
        out_specs=VMEM,
        scratch_shapes=[pltpu.VMEM((rows, LANES), F32), pltpu.VMEM((rows, tokens), F32)],
        compiler_params=limit(12),
        name="lookup",
    )(ids, table)


def tdot(a, b):
    return lax.dot_general(a, b, (((0,), (0,)), ((), ())), preferred_element_type=F32)


def ndot(a, b):
    return lax.dot_general(a, b, (((1,), (1,)), ((), ())), preferred_element_type=F32)


def mdot(a, b):
    return lax.dot_general(a, b, (((1,), (0,)), ((), ())), preferred_element_type=F32)


SLOT = 64
AT_TAPS, AT_ACCEPTED, AT_BIAS, AT_RATE, AT_SKIP = 24, 32, 33, 34, 35


def saved_at(j, kept, seqs, draft):
    seq = lax.broadcasted_iota(jnp.int32, (seqs, seqs * draft), 0)
    at = lax.broadcasted_iota(jnp.int32, (seqs, seqs * draft), 1)
    return (at == seq * draft + (draft - kept) + j).astype(F32).astype(BF)


def setup_kernel(
    bias_ref, rate_ref, skip_ref, w_ref, wdt_ref, state_ref, taps_ref, tapb_ref, gain_ref,
    xtaps_ref, xtapb_ref, gate_ref, statex_ref, accepted_ref,
    vocab_ref,
    keep_ref, send_ref, table_ref, own8_ref, beforex_ref, beforebc_ref, spread_ref, near_ref,
    table, sem,
):
    bring = pltpu.make_async_copy(vocab_ref, near_ref, sem)
    bring.start()
    model = w_ref.shape[2]
    here = w_ref.shape[1]
    kept, seqs = state_ref.shape[1], state_ref.shape[3]
    draft = spread_ref.shape[1] // seqs
    taps = taps_ref.shape[1]
    width = xtaps_ref.shape[2]
    first = position()[2] == 0
    places = [saved_at(j, kept, seqs, draft) for j in range(kept)]
    outs, rows = [], []
    for layer in range(LAYERS):
        table[...] = jnp.zeros_like(table)
        table[0:taps, 0:here] = taps_ref[layer].astype(F32)
        table[taps : taps + 1, 0:here] = tapb_ref[layer : layer + 1].astype(F32)
        turned = jnp.transpose(table[...])[:8]
        tiles = []
        for j in range(kept):
            table[...] = jnp.zeros_like(table)
            table[0:here, 0:seqs] = state_ref[layer, j].astype(F32)
            tiles.append(table[0:8, :])
        outs.append((turned, tiles[0] + pltpu.roll(tiles[1], SLOT, 1), tiles[2]))
        row = w_ref[layer].astype(F32)
        rows.append(jnp.concatenate([row, jnp.zeros((8 - here, model), F32)], axis=0))
        own8_ref[layer] = jnp.concatenate(
            [row, wdt_ref[layer : layer + 1, :].astype(F32), jnp.zeros((7 - here, model), F32)], axis=0
        ).astype(BF)
    for ref, pick in ((keep_ref, first), (send_ref, jnp.logical_not(first))):
        for lo, values in (
            (0, rows),
            (model, [o[0] for o in outs]),
            (model + LANES, [o[1] for o in outs]),
            (model + 2 * LANES, [o[2] for o in outs]),
        ):
            value = jnp.where(pick, values[0], values[1])
            value = jnp.where(first, value, pltpu.roll(value, here, 0))
            ref[:, lo : lo + value.shape[1]] = value.astype(BF)
    for layer in range(LAYERS):
        table[...] = jnp.zeros_like(table)
        for j in range(model // LANES):
            table[j : j + 1, :] = gain_ref[layer : layer + 1, j * LANES : (j + 1) * LANES]
        table[AT_TAPS : AT_TAPS + taps, :width] = xtaps_ref[layer].astype(F32)
        table[AT_TAPS + taps : AT_TAPS + taps + 1, :width] = xtapb_ref[layer : layer + 1].astype(F32)
        table[AT_TAPS + taps + 1 : AT_TAPS + taps + 2, :width] = gate_ref[layer : layer + 1]
        table[AT_ACCEPTED : AT_ACCEPTED + 1, :seqs] = accepted_ref[...].astype(F32)
        table[AT_BIAS : AT_BIAS + 1, :] = jnp.broadcast_to(bias_ref[0:1, layer : layer + 1], (1, LANES))
        table[AT_RATE : AT_RATE + 1, :] = jnp.broadcast_to(rate_ref[0:1, layer : layer + 1], (1, LANES))
        table[AT_SKIP : AT_SKIP + 1, :] = jnp.broadcast_to(skip_ref[0:1, layer : layer + 1], (1, LANES))
        table_ref[layer] = jnp.transpose(table[...])
        beforex_ref[layer] = sum(tdot(statex_ref[layer, j], places[j]) for j in range(kept)).astype(BF)
        beforebc_ref[layer] = jnp.concatenate(
            [
                sum(mdot(state_ref[layer, j], places[j]) for j in range(kept)),
                jnp.zeros((8 - here, seqs * draft), F32),
            ],
            axis=0,
        ).astype(BF)
    seq = lax.broadcasted_iota(jnp.int32, (seqs, seqs * draft), 0)
    at = lax.broadcasted_iota(jnp.int32, (seqs, seqs * draft), 1)
    owner = (at // draft == seq).astype(F32).astype(BF)
    spread_ref[...] = mdot(
        jnp.broadcast_to(accepted_ref[...].astype(F32), (8, seqs)).astype(BF), owner
    ).astype(jnp.int32)
    bring.wait()


def pair_kernel(keep_ref, got_ref, rows_ref):
    rows_ref[...] = (keep_ref[...].astype(F32) + got_ref[...].astype(F32)).astype(BF)


def convolve(now, before, weights, bias, draft):
    tokens = now.shape[1]
    taps = len(weights)
    t0 = lax.broadcasted_iota(jnp.int32, (1, tokens), 1) % draft
    acc = None
    for k in range(taps):
        d = taps - 1 - k
        shifted = now
        if d:
            shifted = jnp.where(
                t0 >= d, pltpu.roll(now, d, 1), pltpu.roll(before, tokens - (draft - d), 1)
            )
        term = shifted * weights[k]
        acc = term if acc is None else acc + term
    return silu(acc + bias)


def make_project_kernel(layer, tokens, seqs, draft, own_cols, taps):
    model = own_cols * YS * ZS * CS
    pieces = own_cols // 8
    kept = taps - 1

    def kernel(
        own_ref, oth_ref, wown_ref, woth_ref, table_ref, own8_ref, nb_ref, mine_ref, bcc_ref, xs
    ):
        core = position()[2]
        first = core == 0
        turned = table_ref[layer]

        total = jnp.zeros((8, tokens), F32)
        for k in range(YS * ZS):
            for j in range(pieces):
                lanes = slice(j * tokens, (j + 1) * tokens)
                a = own_ref[k, :, lanes].astype(F32)
                b = oth_ref[k, :, lanes].astype(F32)
                total = total + a * a + b * b
                at = 2 * k * own_cols + 8 * j
                xs[at : at + 8, :] = jnp.where(first, a, b)
                xs[at + own_cols : at + own_cols + 8, :] = jnp.where(first, b, a)
        scale = lax.rsqrt(jnp.sum(total, axis=0, keepdims=True) / model + EPS)
        for j in range(model // LANES):
            at = slice(j * LANES, (j + 1) * LANES)
            nb_ref[at, :] = ((xs[at, :] * scale) * turned[:, j : j + 1]).astype(BF)

        take_own = core == layer
        count = ZS * 8
        rows = jnp.where(take_own, wown_ref[...].astype(F32), woth_ref[...].astype(F32)).reshape(
            count, model + 3 * LANES
        )
        left = jnp.concatenate([rows[:, :model], own8_ref[layer].astype(F32)], axis=0).astype(BF)
        out = mdot(left, nb_ref[...]).astype(BF)
        mine_ref[...] = out[count:]
        slot = lax.broadcasted_iota(jnp.int32, (2 * LANES, tokens), 0)
        slot_lane = lax.broadcasted_iota(jnp.int32, (2 * LANES, tokens), 1)
        slot_seq, slot_j = slot & (SLOT - 1), slot // SLOT
        place = (
            (slot_seq < seqs) & (slot_j < kept) & (slot_lane == slot_seq * draft + (draft - kept) + slot_j)
        ).astype(F32).astype(BF)
        before = mdot(rows[:, model + LANES :].astype(BF), place)
        extra = rows[:, model : model + LANES]
        bcc = convolve(
            out[:count].astype(F32),
            before,
            [extra[:, k : k + 1] for k in range(taps)],
            extra[:, taps : taps + 1],
            draft,
        )
        bcc_ref[...] = bcc.astype(BF)

    return kernel


def make_values_kernel(layer, tokens, seqs, draft, taps, last):
    kept = taps - 1

    def kernel(*refs):
        (
            nb_ref, mine_ref, table_ref, beforex_ref, beforebc_ref, spread_ref, zx_ref,
            ssm_ref, *rest,
        ) = refs
        if last:
            old_x_ref, old_bc_ref, *rest = rest
        gate_ref, xc_ref, rows_ref, h_ref, newx_ref, newbc_ref, zx_w, sems = rest
        load_w = pltpu.make_async_copy(zx_ref.at[layer], zx_w, sems.at[0])
        load_h = pltpu.make_async_copy(ssm_ref.at[layer], h_ref, sems.at[1])
        load_w.start()
        load_h.start()
        turned = table_ref[layer]
        width = beforex_ref.shape[1]
        here = newbc_ref.shape[-2]
        acc_col = turned[:seqs, AT_ACCEPTED : AT_ACCEPTED + 1].astype(jnp.int32)
        cols = turned[:width, AT_TAPS : AT_TAPS + 8]
        bias_dt = turned[:1, AT_BIAS : AT_BIAS + 1]
        rate = turned[:1, AT_RATE : AT_RATE + 1]
        lane = lax.broadcasted_iota(jnp.int32, (1, tokens), 1)
        t0 = lane % draft
        mine = mine_ref[...]
        before_b, before_mb = beforex_ref[layer], beforebc_ref[layer]

        step = softplus(mine[here : here + 1, :].astype(F32) + bias_dt)
        cum = step
        for d in (1, 2, 4):
            cum = cum + jnp.where(t0 >= d, pltpu.roll(cum, d, 1), 0.0)
        accepted = spread_ref[:1]
        cut = jnp.where(t0 < accepted, step, 0.0)
        for d in (1, 2, 4):
            cut = cut + jnp.where((t0 & d) != 0, pltpu.roll(cut, d, 1), pltpu.roll(cut, tokens - d, 1))
        weight = jnp.where(t0 < accepted, jnp.exp(-rate * (cut - cum)) * step, 0.0)
        rows = (step, cum, jnp.exp(-rate * cum), jnp.exp(-rate * cut), weight)
        for i, row in enumerate(rows):
            rows_ref[i : i + 1, :] = row
        rows_ref[len(rows) :, :] = jnp.zeros((8 - len(rows), tokens), F32)

        load_w.wait()
        zx = tdot(zx_w[...], nb_ref[...]).astype(BF)
        gate_ref[...] = silu(zx[:width].astype(F32))
        values_b = zx[width:]
        xc_ref[...] = convolve(
            values_b.astype(F32),
            before_b.astype(F32),
            [cols[:, k : k + 1] for k in range(taps)],
            cols[:, taps : taps + 1],
            draft,
        )

        seq = lax.broadcasted_iota(jnp.int32, (seqs, tokens), 0)
        at = lax.broadcasted_iota(jnp.int32, (seqs, tokens), 1)
        for i in range(kept):
            row = acc_col + i
            new = ((at == seq * draft + row - kept) & (row >= kept)).astype(F32).astype(BF)
            old = ((at == seq * draft + (draft - kept) + row) & (row < kept)).astype(F32).astype(BF)
            rows_x = (ndot(new, values_b) + ndot(old, before_b)).astype(BF)
            rows_bc = (ndot(mine, new) + ndot(before_mb, old))[:here].astype(BF)
            if last:
                newx_ref[layer, i], newbc_ref[layer, i] = rows_x, rows_bc
                for l in range(layer):
                    newx_ref[l, i], newbc_ref[l, i] = old_x_ref[i], old_bc_ref[i]
            else:
                newx_ref[i], newbc_ref[i] = rows_x, rows_bc
        load_h.wait()

    return kernel


def make_recur_kernel(layer, tokens, draft, own_cols, taps, last):
    pieces = own_cols // 8

    def kernel(*refs):
        got_refs = refs[:YS]
        gate_ref, xc_ref, rows_ref, h_in, table_ref, outw_ref, *rest = refs[YS:]
        if last:
            _, *rest = rest
        keep_ref, send_ref, newssm_ref, h_out, xw_all, out_w, channels, sems = rest
        y_here, _, core = position()
        first = core == 0
        load_o = pltpu.make_async_copy(outw_ref.at[layer], out_w, sems.at[0])
        load_o.start()
        turned = table_ref[layer]
        width = xc_ref.shape[0]
        rate = turned[:1, AT_RATE : AT_RATE + 1]
        skip = turned[:1, AT_SKIP : AT_SKIP + 1]
        gain = turned[:width, AT_TAPS + taps + 1 : AT_TAPS + taps + 2]
        xc = xc_ref[...]
        step, cum, fall, fall_cut, weight = [rows_ref[i : i + 1, :] for i in range(5)]
        for d, ref in enumerate(got_refs):
            channels[lax.rem(y_here + d, YS)] = ref[...].astype(F32)
        bcc = channels[...].reshape(-1, xc_ref.shape[1]).astype(BF)
        states = bcc.shape[0] // 2
        xb = xc.astype(BF)
        xw_all[...] = (xc * weight).astype(BF)

        per_tile = LANES // draft
        sub = lax.broadcasted_iota(jnp.int32, (LANES, LANES), 0)
        lan = lax.broadcasted_iota(jnp.int32, (LANES, LANES), 1)
        causal = (sub // draft == lan // draft) & (sub <= lan)
        group = lax.broadcasted_iota(jnp.int32, (1, LANES), 1) // draft
        pick16 = lax.broadcasted_iota(jnp.int32, (per_tile, LANES), 0) * draft == (
            lax.broadcasted_iota(jnp.int32, (per_tile, LANES), 1)
        )
        parts = []
        for tile in range(tokens // LANES):
            ls = slice(tile * LANES, (tile + 1) * LANES)
            bmat = bcc[:states, ls]
            cmat = bcc[states:, ls]
            cum_r = jnp.broadcast_to(cum[:, ls], (LANES, LANES))
            step_c = jnp.transpose(jnp.broadcast_to(step[:, ls], (LANES, LANES)))
            cum_c = jnp.transpose(cum_r)
            gram = tdot(bmat, cmat)
            within = jnp.where(causal, gram * (jnp.exp(-rate * (cum_r - cum_c)) * step_c), 0.0)
            y_new = mdot(xb[:, ls], within.astype(BF))
            y_old = jnp.zeros((width, LANES), F32)
            falls = jnp.sum(jnp.where(pick16, fall_cut[:, ls], 0.0), axis=1, keepdims=True)
            xw = xw_all[:, ls]
            for s in range(per_tile):
                n = tile * per_tile + s
                h0 = h_in[n]
                here = group == s
                y_old = jnp.where(here, mdot(h0.astype(BF), cmat), y_old)
                add = ndot(jnp.where(here, xw, jnp.zeros_like(xw)), bmat)
                h_out[n] = h0 * falls[s : s + 1, :] + add
            parts.append(fall[:, ls] * y_old + y_new)
        store = pltpu.make_async_copy(h_out, newssm_ref.at[layer], sems.at[1])
        store.start()
        y = jnp.concatenate(parts, axis=1) + skip * xc
        gated = y * gate_ref[...]
        ssq = jnp.sum(gated * gated, axis=0, keepdims=True)
        u = (gated * gain).astype(BF)

        high = ssq.astype(BF)
        low = (ssq - high.astype(F32)).astype(BF)
        row8 = lax.broadcasted_iota(jnp.int32, (8, tokens), 0)
        tail = jnp.where(row8 == 0, high.astype(F32), jnp.where(row8 == 1, low.astype(F32), 0.0))
        block = own_cols * CS * ZS
        load_o.wait()
        for y_at in range(YS):
            out = tdot(out_w[:, y_at * block : (y_at + 1) * block], u)
            out = out.reshape(ZS, CS, pieces, 8, tokens)
            for z in range(ZS):
                even, odd = out[z, 0], out[z, 1]
                rows = slice(z * pieces, (z + 1) * pieces)
                keep_ref[y_at, rows] = jnp.where(first, even, odd)
                send_ref[y_at, rows] = jnp.where(first, odd, even).astype(BF)
            keep_ref[y_at, ZS * pieces] = tail
            send_ref[y_at, ZS * pieces] = tail.astype(BF)
        store.wait()

    return kernel


def add_cores_kernel(keep_ref, got_ref, *out_refs):
    tiles = keep_ref.shape[1]
    y, _, core = position()
    turn = jnp.where(core == 0, 1, YS - 1)
    tail = split_tail(keep_ref[0, tiles - 1] + got_ref[0, tiles - 1].astype(F32))
    for shift, out_ref in enumerate(out_refs):
        at = lax.rem(y + shift * turn, YS)
        out_ref[: tiles - 1] = (
            keep_ref[at, : tiles - 1] + got_ref[at, : tiles - 1].astype(F32)
        ).astype(BF)
        out_ref[tiles - 1] = tail


def split_tail(tail):
    row8 = lax.broadcasted_iota(jnp.int32, tail.shape, 0)
    ssq = tail[0:1] + tail[1:2]
    high = ssq.astype(BF).astype(F32)
    return jnp.where(row8 == 0, high, jnp.where(row8 == 1, ssq - high, 0.0)).astype(BF)


def add_y_kernel(*refs):
    *got_refs, out_ref = refs
    tiles = got_refs[0].shape[0]
    pieces = (tiles - 1) // ZS

    def summed(rows):
        acc = got_refs[0][rows].astype(F32)
        for ref in got_refs[1:]:
            acc = acc + ref[rows].astype(F32)
        return acc

    tail = split_tail(summed(slice(tiles - 1, tiles))[0])
    for z in range(ZS):
        out_ref[z, :pieces] = summed(slice(z * pieces, (z + 1) * pieces)).astype(BF)
        out_ref[z, pieces] = tail


def make_finish_kernel(inner, last):
    def finish_kernel(got_ref, stream_ref, out_ref):
        tiles = got_ref.shape[1]
        tokens = got_ref.shape[3]
        acc = got_ref[0].astype(F32)
        for z in range(1, ZS):
            acc = acc + got_ref[z].astype(F32)
        ssq = acc[tiles - 1, 0:1] + acc[tiles - 1, 1:2]
        scale = lax.rsqrt(ssq / inner + EPS)
        for j in range(tiles - 1):
            lanes = slice(j * tokens, (j + 1) * tokens)
            new = (stream_ref[:, lanes].astype(F32) + acc[j] * scale).astype(BF)
            if last:
                out_ref[j] = new
            else:
                out_ref[:, lanes] = new

    return finish_kernel


def call(kernel, out_shape, count):
    return pl.pallas_call(
        kernel,
        out_shape=out_shape,
        in_specs=[VMEM] * count,
        out_specs=jax.tree.map(lambda _: VMEM, out_shape),
        compiler_params=limit(10),
    )


def local(
    draft_ids,
    accepted,
    embedding,
    norm_gain,
    w_zx,
    w_dt,
    w_bc,
    dt_bias,
    decay_rate,
    skip_weight,
    conv_x_w,
    conv_x_b,
    conv_bc_w,
    conv_bc_b,
    gate_gain,
    out_w,
    ssm_state,
    conv_x_state,
    conv_bc_state,
):
    seqs, draft = draft_ids.shape
    tokens = seqs * draft
    own_cols = embedding.shape[1]
    model = own_cols * YS * ZS * CS
    width = w_zx.shape[3] // 2
    inner = width * YS * ZS * CS
    bc_here = w_bc.shape[2]
    taps = conv_x_w.shape[1]
    kept = taps - 1
    pieces = own_cols // 8
    states = ssm_state.shape[4]

    tokens_ids = draft_ids.T
    state_shape = (LAYERS, seqs, width, states)

    w_rows = jnp.swapaxes(w_bc, 1, 2)
    row_shape = jax.ShapeDtypeStruct((8, model + 3 * LANES), BF)
    keep, send, table, own8, before_x, before_bc, spread_acc, vocab = pl.pallas_call(
        setup_kernel,
        out_shape=(
            row_shape,
            row_shape,
            jax.ShapeDtypeStruct((LAYERS, LANES, LANES), F32),
            jax.ShapeDtypeStruct((LAYERS, 8, model), BF),
            jax.ShapeDtypeStruct((LAYERS, width, tokens), BF),
            jax.ShapeDtypeStruct((LAYERS, 8, tokens), BF),
            jax.ShapeDtypeStruct((8, tokens), jnp.int32),
            jax.ShapeDtypeStruct(embedding.shape[::-1], BF),
        ),
        in_specs=[VMEM] * 14 + [HBM],
        out_specs=(VMEM,) * 8,
        scratch_shapes=[pltpu.VMEM((LANES, LANES), F32), pltpu.SemaphoreType.DMA],
        compiler_params=limit(16),
        name="setup",
    )(
        *[
            pltpu.with_memory_space_constraint(v, pltpu.HBM)
            for v in (
                *[v.reshape(1, LAYERS) for v in (dt_bias, decay_rate, skip_weight)],
                w_rows,
                w_dt.reshape(LAYERS, model),
                jnp.transpose(conv_bc_state, (0, 2, 3, 1)),
                conv_bc_w,
                conv_bc_b,
                norm_gain,
                conv_x_w,
                conv_x_b,
                gate_gain,
                jnp.swapaxes(conv_x_state, 1, 2),
                accepted.reshape(1, seqs),
                embedding.T,
            )
        ],
    )
    pair_rows = call(pair_kernel, row_shape, 2)(keep, swap_cores(send))
    stream = lookup(tokens_ids, vocab)
    w_own = spread(pair_rows, Z_GROUPS)
    w_oth = swap_cores(w_own)
    own, oth = gather_planes(stream)

    zx_w, outer_w, state_in = [
        pltpu.with_memory_space_constraint(v, pltpu.HBM)
        for v in (w_zx.reshape(LAYERS, model, 2 * width), out_w, ssm_state.reshape(state_shape))
    ]
    saved, saved_ssm = (), ()
    tiles = ZS * pieces + 1
    for layer in range(LAYERS):
        last = layer + 1 == LAYERS
        lead = (LAYERS,) if last else ()
        normed, mine, bcc = pl.pallas_call(
            make_project_kernel(layer, tokens, seqs, draft, own_cols, taps),
            out_shape=(
                jax.ShapeDtypeStruct((model, tokens), BF),
                jax.ShapeDtypeStruct((8, tokens), BF),
                jax.ShapeDtypeStruct((ZS * 8, tokens), BF),
            ),
            in_specs=[VMEM] * 6,
            out_specs=(VMEM,) * 3,
            scratch_shapes=[pltpu.VMEM((model, tokens), F32)],
            compiler_params=limit(14),
        )(own, oth, w_own, w_oth, table, own8)
        got = [bcc] + [from_y(bcc, d) for d in range(1, YS)]
        gate, xc, rows, h_in, *saved = pl.pallas_call(
            make_values_kernel(layer, tokens, seqs, draft, taps, last),
            out_shape=(
                jax.ShapeDtypeStruct((width, tokens), F32),
                jax.ShapeDtypeStruct((width, tokens), F32),
                jax.ShapeDtypeStruct((8, tokens), F32),
                jax.ShapeDtypeStruct(state_shape[1:], F32),
                jax.ShapeDtypeStruct((*lead, kept, seqs, width), BF),
                jax.ShapeDtypeStruct((*lead, kept, bc_here, seqs), BF),
            ),
            in_specs=[VMEM] * 6 + [HBM] * 2 + [VMEM] * len(saved),
            out_specs=(VMEM,) * 6,
            scratch_shapes=[
                pltpu.VMEM((model, 2 * width), BF),
                pltpu.SemaphoreType.DMA((2,)),
            ],
            compiler_params=limit(10),
            cost_estimate=pl.CostEstimate(
                flops=2 * model * tokens * 4 * width, bytes_accessed=4 << 20, transcendentals=0
            ),
        )(
            normed, mine, table, before_x, before_bc, spread_acc, zx_w, state_in, *saved
        )
        keep, send, *saved_ssm = pl.pallas_call(
            make_recur_kernel(layer, tokens, draft, own_cols, taps, last),
            out_shape=(
                jax.ShapeDtypeStruct((YS, tiles, 8, tokens), F32),
                jax.ShapeDtypeStruct((YS, tiles, 8, tokens), BF),
                jax.ShapeDtypeStruct(state_shape, F32),
            ),
            in_specs=[VMEM] * 9 + [HBM] * (1 + len(saved_ssm)),
            out_specs=(VMEM, VMEM, HBM),
            scratch_shapes=[
                pltpu.VMEM(state_shape[1:], F32),
                pltpu.VMEM((width, tokens), BF),
                pltpu.VMEM((width, model), BF),
                pltpu.VMEM((YS, ZS * 8, tokens), F32),
                pltpu.SemaphoreType.DMA((2,)),
            ],
            input_output_aliases={10: 2} if last else {},
            compiler_params=limit(14),
        )(*got, gate, xc, rows, h_in, table, outer_w, *saved_ssm)
        block = jax.ShapeDtypeStruct((tiles, 8, tokens), BF)
        here, *blocks = call(add_cores_kernel, (block,) * YS, 2)(keep, swap_cores(send))
        got = {d: to_y(blocks[d - 1], d) for d in range(1, YS)}
        summed = call(
            add_y_kernel, jax.ShapeDtypeStruct((ZS, pieces + 1, 8, tokens), BF), YS
        )(here, *[got[d] for d in range(1, YS)])
        shape = (pieces, 8, tokens) if last else (8, pieces * tokens)
        stream = call(
            make_finish_kernel(inner, last), jax.ShapeDtypeStruct(shape, BF), 2
        )(exchange(summed, Z_GROUPS), stream)
        if not last:
            own, oth = gather_planes(stream)
    (new_x, new_bc), (new_ssm,) = saved, saved_ssm
    hidden = stream.reshape(own_cols, tokens).T
    kept_x = jnp.swapaxes(new_x, 1, 2)
    kept_bc = jnp.transpose(new_bc, (0, 3, 1, 2))
    return (hidden, new_ssm.reshape(ssm_state.shape), kept_x, kept_bc)


def solution(mesh):
    placed = (
        P("batch", None),
        P("batch"),
        P(None, "heads"),
        P(),
        P(None, None, "heads", None),
        P(None, None, "heads"),
        P(None, None, "heads"),
        P(None, "heads"),
        P(None, "heads"),
        P(None, "heads"),
        P(None, None, "heads"),
        P(None, "heads"),
        P(None, None, "heads"),
        P(None, "heads"),
        P(None, "heads"),
        P(None, "heads", None),
        P(None, "batch", "heads", None, None),
        P(None, "batch", None, "heads"),
        P(None, "batch", None, "heads"),
    )
    return jax.shard_map(
        local,
        mesh=mesh,
        in_specs=placed,
        out_specs=(
            P("batch", "heads"),
            P(None, "batch", "heads", None, None),
            P(None, "batch", None, "heads"),
            P(None, "batch", None, "heads"),
        ),
        check_vma=False,
    )
```
